32 devices in a mesh: row: 8 (over z, x), col: 4 (over y, core).
Axes of the slice: x: 2, y: 2, z: 4, core: 2. Of those that a mesh axis runs over, the one named last changes fastest.
Arguments:
- dense_a: bfloat16 [64, 512, 512], P(('row', 'col')), may hold values from -6 to 6
- dense_b: bfloat16 [64, 512, 512], P(('row', 'col')), may hold values from -0.25 to 0.25
- inner_basis_stack: bfloat16 [64, 2, 512, 128], P(('row', 'col')), may hold values from -0.25 to 0.25
- outer_basis_stack: bfloat16 [64, 2, 512, 128], P(('row', 'col')), may hold values from -1 to 1
- ascent: bfloat16 [32, 4, 2, 128, 128], P(('row', 'col')), may hold values from -0.4375 to 0.4375
- descent: bfloat16 [32, 4, 2, 128, 128], P(('row', 'col')), may hold values from -0.5 to 0.5
- couplings: bfloat16 [32, 2, 4, 128, 128], P(('row', 'col')), may hold values from -0.5 to 0.5
Outputs:
- product_diag: bfloat16 [64, 512, 512], P(('row', 'col'))
The draws below stay inside these ranges and needn't reach their ends.
All inputs are finite; a program needn't handle non-finite values.
Results may differ from the reference program's by a relative error of at most 0.015.
Values may be sent and summed in bfloat16 or wider, within the bound.
No kernel may reach another device: no remote copies, remote signals or barrier semaphores. Data moves between devices by JAX's collectives and lax.ppermute only.
A program may use at most 64 MiB of HBM per device.

```python
import jax
import jax.numpy as jnp
from jax import lax

M = 512
R = 128
DEVICES_ALL = 32
LEAVES = 64
N_ROW = 8
N_COL = 4


def block_scale(rng, extent, shards, low, largest):
    level, own = 1.0, jax.random.fold_in(rng, 6)
    for position, shards_of in shards:
        draws = jnp.exp(jax.random.uniform(jax.random.fold_in(own, position), (shards_of,), jnp.float32, low / len(shards), largest / len(shards)))
        level = level * jnp.repeat(draws, extent[position] // shards_of).reshape([-1 if axis == position else 1 for axis in range(len(extent))])
    return level


def scatter_about(own_key, dims, width, reach, shards=(), kind=jnp.bfloat16):
    factor_of = block_scale(own_key, dims, shards, -0.22, 0.18) if shards else 1.0
    drawn = jax.random.normal(own_key, dims, jnp.float32) * width * factor_of
    return jnp.minimum(jnp.maximum(drawn, -reach), reach).astype(kind)


def setup_inputs(seed: int = 0) -> dict:
    keys = jax.random.split(jax.random.key(seed), 8)
    dense_a = scatter_about(keys[0], (LEAVES, M, M), 1.0, 6.0, ((0, 32),))
    dense_b = scatter_about(keys[1], (LEAVES, M, M), M ** -0.5, 0.25, ((0, 32),))
    inner_basis_stack = scatter_about(keys[2], (LEAVES, 2, M, R), M ** -0.5, 0.25, ((0, 32),))
    outer_basis_stack = scatter_about(keys[3], (LEAVES, 2, M, R), (R // 4) ** -0.5, 1.0, ((0, 32),))
    ascent = scatter_about(keys[4], (DEVICES_ALL, 4, 2, R, R), (R * 7 // 5) ** -0.5, 0.4375, ((0, 32),))
    descent = scatter_about(keys[5], (DEVICES_ALL, 4, 2, R, R), R ** -0.5, 0.5, ((0, 32),))
    couplings = scatter_about(keys[6], (DEVICES_ALL, 2, 4, R, R), R ** -0.5, 0.5, ((0, 32),))
    return {"dense_a": dense_a, "dense_b": dense_b, "inner_basis_stack": inner_basis_stack, "outer_basis_stack": outer_basis_stack, "ascent": ascent, "descent": descent, "couplings": couplings}


HIGHEST_PRECISION = lax.Precision.HIGHEST


def multiply(first_arg, second_arg):
    return jnp.matmul(first_arg.astype(jnp.float32), second_arg.astype(jnp.float32), precision=HIGHEST_PRECISION)


def lifted(pair_stack, inner_value):
    return multiply(multiply(jnp.swapaxes(pair_stack[:, 0], 1, 2), inner_value), pair_stack[:, 1])


def lowered(pair_stack, parent):
    return multiply(multiply(pair_stack[:, 0], parent), jnp.swapaxes(pair_stack[:, 1], 1, 2))


def sibling_terms(blocks, inner_value):
    left_terms = multiply(multiply(blocks[:, 0], inner_value[1::2]), blocks[:, 3])
    right_terms = multiply(multiply(blocks[:, 1], inner_value[0::2]), blocks[:, 2])
    return jnp.stack([left_terms, right_terms], 1).reshape(inner_value.shape)


def owners(stacked, height):
    return stacked[2 ** (height - 1) - 1::2 ** height]


def leaf_block(leaf_items):
    first_matrix_block, block_b, bases, mixing = leaf_items
    spread_rows = jnp.dot(bases[0], mixing, preferred_element_type=jnp.float32).astype(jnp.bfloat16)
    result_block = jnp.dot(first_matrix_block, block_b, preferred_element_type=jnp.float32)
    result_block = result_block + jnp.dot(spread_rows, bases[1].T, preferred_element_type=jnp.float32)
    return result_block.astype(jnp.bfloat16)


def reference(dense_a, dense_b, inner_basis_stack, outer_basis_stack, ascent, descent, couplings):
    device_list = N_ROW * N_COL
    levels = device_list.bit_length() - 1
    leaf_inner_product = jnp.einsum('ufw,ufa->uwa', inner_basis_stack[:, 0].astype(jnp.float32),
                            inner_basis_stack[:, 1].astype(jnp.float32), precision=HIGHEST_PRECISION)
    leaf_up = ascent[:, 0:2].reshape(2 * device_list, 2, R, R)
    inner_levels = [leaf_inner_product]
    lifted_terms = lifted(leaf_up, leaf_inner_product)
    current = lifted_terms[0::2] + lifted_terms[1::2]
    inner_levels.append(current)
    for height in range(1, levels + 1):
        if height == 1:
            pair_stack = ascent[:, 2]
        else:
            pair_stack = owners(ascent[:, 3], height - 1)
        lifted_terms = lifted(pair_stack, current)
        current = lifted_terms[0::2] + lifted_terms[1::2]
        inner_levels.append(current)
    coupling = jnp.zeros((1, R, R), jnp.float32)
    for height in range(levels, 0, -1):
        near_terms = sibling_terms(owners(couplings[:, 1], height), inner_levels[height])
        if height == 1:
            pair_stack = descent[:, 2]
        else:
            pair_stack = owners(descent[:, 3], height - 1)
        coupling = near_terms + lowered(pair_stack, jnp.repeat(coupling, 2, axis=0))
    near_terms = sibling_terms(couplings[:, 0], leaf_inner_product)
    leaf_down = descent[:, 0:2].reshape(2 * device_list, 2, R, R)
    leaf_coupling = near_terms + lowered(leaf_down, jnp.repeat(coupling, 2, axis=0))
    rounded_count = leaf_coupling.astype(jnp.bfloat16)
    return lax.map(leaf_block, (dense_a, dense_b, outer_basis_stack, rounded_count))
```

```python
import functools

import jax
import jax.numpy as jnp
from jax import lax
from jax.experimental import pallas as pl
from jax.experimental.pallas import tpu as pltpu
from jax.sharding import PartitionSpec as P

AXES = ("row", "col")
BF16 = jnp.bfloat16
F32 = jnp.float32
VMEM = pltpu.VMEM


def dot(a, b):
    return lax.dot_general(a, b, (((1,), (0,)), ((), ())), preferred_element_type=F32)


def dot_tn(a, b):
    return lax.dot_general(a, b, (((0,), (0,)), ((), ())), preferred_element_type=F32)


def dot_nt(a, b):
    return lax.dot_general(a, b, (((1,), (1,)), ((), ())), preferred_element_type=F32)


def lift(p, f, q):
    return dot(dot_tn(p, f).astype(BF16), q)


def couple(k, f, k2):
    return dot(dot(k, f).astype(BF16), k2)


def lower(s, g, w):
    return dot_nt(dot(s, g).astype(BF16), w)


def leaf_kernel(inner_ref, up_ref, leaf_ref, pair_ref):
    total = None
    for i in range(2):
        f = dot_tn(inner_ref[i, 0], inner_ref[i, 1]).astype(BF16)
        leaf_ref[i] = f
        t = lift(up_ref[i, 0], f, up_ref[i, 1])
        total = t if total is None else total + t
    f0 = total.astype(BF16)
    pair_ref[0] = f0
    pair_ref[1] = lift(up_ref[2, 0], f0, up_ref[2, 1]).astype(BF16)


def final_kernel(levels, *refs):
    side_ref, leaf_ref, down_ref, block_ref = refs[:4]
    sib_refs = refs[4 : 4 + levels]
    k_refs = refs[4 + levels : 4 + 2 * levels]
    sw_refs = refs[4 + 2 * levels : 4 + 3 * levels - 2]
    dense_ref, outer_ref, out_ref = refs[4 + 3 * levels - 2 :]
    coupling = None
    for height in range(levels, 0, -1):
        side = side_ref[height - 1]
        k = k_refs[height - 1]
        near = couple(k[side], sib_refs[height - 1][0], k[3 - side])
        if coupling is None:
            coupling = near
        else:
            g = coupling.astype(BF16)
            if height >= 2:
                sw = sw_refs[height - 2]
                coupling = near + lower(sw[0], g, sw[1])
            else:
                coupling = near + lower(down_ref[2, 0], g, down_ref[2, 1])
    g = coupling.astype(BF16)
    for i in range(2):
        near = couple(block_ref[i], leaf_ref[1 - i], block_ref[3 - i])
        gb = (near + lower(down_ref[i, 0], g, down_ref[i, 1])).astype(BF16)
        e = dot(outer_ref[i, 0], gb).astype(BF16)
        out_ref[i] = (dense_ref[i] + dot_nt(e, outer_ref[i, 1])).astype(BF16)


def vmem_specs(n):
    return [pl.BlockSpec(memory_space=VMEM)] * n


def exchange(block, distance, count, odd_only=False, low_only=False):
    route = []
    for p in range(count):
        if odd_only and p % 2 == 0:
            continue
        if low_only and p & distance:
            continue
        route.append((p, p ^ distance))
    return lax.ppermute(block, AXES, route)


def shards(dense_a, dense_b, inner_basis_stack, outer_basis_stack, ascent, descent, couplings):
    count = lax.axis_size("row") * lax.axis_size("col")
    levels = count.bit_length() - 1
    rank = ascent.shape[-1]
    position = lax.axis_index(AXES)
    up, down, blocks = ascent[0], descent[0], couplings[0]

    own = jnp.concatenate([up[3], down[3], blocks[1]], 0)

    def bit(b):
        return (position >> b) & 1

    def swap_cores(block):
        return exchange(block, 1, count)

    mat = jax.ShapeDtypeStruct((2, rank, rank), BF16)
    nodes = [None] * levels
    with jax.named_scope("gens_y"):
        carry = own
        got = exchange(carry, 2, count, odd_only=True)
    with jax.named_scope("gens_core"):
        other = swap_cores(own)
    nodes[0] = jnp.where(bit(0) == 0, own, other)

    leaf_inner, pair = pl.pallas_call(
        leaf_kernel,
        out_shape=(mat, mat),
        in_specs=vmem_specs(2),
        out_specs=tuple(vmem_specs(2)),
        name="leaf",
    )(inner_basis_stack, up)

    for b in range(1, levels):
        low = bit(b) == 0
        node = jnp.where(low, carry, got)
        carry = jnp.where(low, got, carry)
        if b + 2 >= levels - 1 and carry.shape[0] == 8:
            carry = carry[4:8]
        if b >= levels - 2:
            node = node[-4:]
        with jax.named_scope(f"gens_fwd_{b}"):
            fwd = exchange(node, 1, count, odd_only=True)
        nodes[b] = jnp.where(bit(0) == 1, node, fwd)
        if b + 1 < levels:
            with jax.named_scope(f"gens_{b + 1}"):
                got = exchange(carry, 1 << (b + 1), count, odd_only=True, low_only=b + 1 == levels - 1)

    dense = lax.dot_general(
        dense_a, dense_b, (((2,), (1,)), ((0,), (0,))), preferred_element_type=F32
    )

    siblings = []
    for b in range(levels):
        with jax.named_scope(f"pair_{b}"):
            received = exchange(pair, 1 << b, count)
        siblings.append(received[0:1])
        if b + 1 < levels:
            inner = pair[1].astype(F32) + received[1].astype(F32)
            f = inner.astype(BF16)
            if b + 2 < levels:
                t = lift(nodes[b][0], f, nodes[b][1]).astype(BF16)
                pair = jnp.stack([f, t])
            else:
                pair = f[None]

    sides = jnp.stack([bit(b) for b in range(levels)]).astype(jnp.int32)
    ks = [node[-4:] for node in nodes]
    sws = [node[2:4] for node in nodes[: levels - 2]]
    n_in = 4 + levels + len(ks) + len(sws) + 2
    return pl.pallas_call(
        functools.partial(final_kernel, levels),
        out_shape=jax.ShapeDtypeStruct(dense.shape, BF16),
        in_specs=[pl.BlockSpec(memory_space=pltpu.SMEM)] + vmem_specs(n_in - 1),
        out_specs=pl.BlockSpec(memory_space=VMEM),
        name="final",
    )(sides, leaf_inner, down, blocks[0], *siblings, *ks, *sws, dense, outer_basis_stack)


def solution(mesh):
    placed = (
        P(AXES, None, None),
        P(AXES, None, None),
        P(AXES, None, None, None),
        P(AXES, None, None, None),
        P(AXES, None, None, None, None),
        P(AXES, None, None, None, None),
        P(AXES, None, None, None, None),
    )
    return jax.shard_map(
        shards, mesh=mesh, in_specs=placed, out_specs=P(AXES, None, None), check_vma=False
    )
```

```python
import functools

import jax
import jax.numpy as jnp
from jax import lax
from jax.experimental import pallas as pl
from jax.experimental.pallas import tpu as pltpu
from jax.sharding import PartitionSpec as P

AXES = ("row", "col")
BF16 = jnp.bfloat16
F32 = jnp.float32
VMEM = pltpu.VMEM


def contract(a, b, left, right):
    return lax.dot_general(a, b, (((left,), (right,)), ((), ())), preferred_element_type=F32)


def dot(a, b):
    return contract(a, b, 1, 0)


def lift(p, f, q):
    return dot(contract(p, f, 0, 0).astype(BF16), q)


def couple(k, f, k2):
    return dot(dot(k, f).astype(BF16), k2)


def lower(s, g, w):
    return contract(dot(s, g).astype(BF16), w, 1, 1)


def pick(first, first_ref, second_ref, i):
    return jnp.where(first, first_ref[i], second_ref[i])


def head_kernel(inner_hbm, up_hbm, down_hbm, block_hbm, swk_ref, leaf_ref, pair_ref, inner, up, sems):
    copies = [
        pltpu.make_async_copy(inner_hbm, inner, sems.at[0]),
        pltpu.make_async_copy(up_hbm.at[0, 0:3], up, sems.at[1]),
        pltpu.make_async_copy(up_hbm.at[0, 3], pair_ref.at[2:4], sems.at[2]),
        pltpu.make_async_copy(down_hbm.at[0, 3], swk_ref.at[0:2], sems.at[3]),
        pltpu.make_async_copy(block_hbm.at[0, 1], swk_ref.at[2:6], sems.at[4]),
    ]
    for copy in copies:
        copy.start()
    copies[0].wait()
    leaves = [contract(inner[i, 0], inner[i, 1], 0, 0).astype(BF16) for i in range(2)]
    copies[1].wait()
    total = None
    for i in range(2):
        leaf_ref[i] = leaves[i]
        t = lift(up[i, 0], leaves[i], up[i, 1])
        total = t if total is None else total + t
    f0 = total.astype(BF16)
    pair_ref[0] = f0
    pair_ref[1] = lift(up[2, 0], f0, up[2, 1]).astype(BF16)
    for copy in copies[2:]:
        copy.wait()


def round_kernel(b, position_ref, pair_ref, received_ref, out_ref):
    low = ((position_ref[0] >> b) & 1) == 0
    f = (pair_ref[1].astype(F32) + received_ref[1].astype(F32)).astype(BF16)
    out_ref[0] = f
    if out_ref.shape[0] > 1:
        p = pick(low, pair_ref, received_ref, 2)
        q = pick(low, pair_ref, received_ref, 3)
        out_ref[1] = lift(p, f, q).astype(BF16)
    if out_ref.shape[0] > 2:
        out_ref[2] = pick(low, received_ref, pair_ref, 2)
        out_ref[3] = pick(low, received_ref, pair_ref, 3)


def carry_kernel(b, position_ref, carry_ref, got_ref, out_ref):
    low = ((position_ref[0] >> b) & 1) == 0
    n = out_ref.shape[0]
    skip = carry_ref.shape[0] - n

    @pl.when(low)
    def _():
        out_ref[...] = got_ref[skip:]

    @pl.when(jnp.logical_not(low))
    def _():
        out_ref[...] = carry_ref[skip:]


def dense_kernel(a_ref, b_ref, o_ref):
    for i in range(2):
        o_ref[i] = dot(a_ref[i], b_ref[i])


def near_term(position, height, carry_ref, got_ref, sibling):
    bit = (position >> (height - 1)) & 1
    base = carry_ref.shape[0] - 4
    left = pick(bit == 0, carry_ref, got_ref, base + bit)
    right = pick(bit == 0, carry_ref, got_ref, base + 3 - bit)
    return couple(left, sibling, right)


def upper_kernel(levels, position_ref, *refs):
    position = position_ref[0]
    received = refs[: levels - 1]
    carries = refs[levels - 1 : 3 * levels - 1 : 2]
    gots = refs[levels : 3 * levels - 1 : 2]
    out_ref = refs[3 * levels - 1]
    coupling = None
    for height in range(levels, 1, -1):
        near = near_term(
            position, height, carries[height - 1], gots[height - 1], received[height - 2][0]
        )
        if coupling is not None:
            low = ((position >> (height - 1)) & 1) == 0
            below = height - 2
            low = ((position >> below) & 1) == 0
            s = pick(low, carries[below], gots[below], 0)
            w = pick(low, carries[below], gots[below], 1)
            near = near + lower(s, coupling, w)
        coupling = near.astype(BF16)
    out_ref[0] = coupling


def final_kernel(
    position_ref, top_ref, got_top_ref, received_ref, carry_ref, got_ref, leaf_ref, down_ref,
    block_ref, dense_ref, outer_ref, out_hbm, out, sems,
):
    position = position_ref[0]
    odd = (position & 1) == 1
    near = near_term(position, 1, carry_ref, got_ref, received_ref[0])
    nears = [couple(block_ref[0, 0, i], leaf_ref[1 - i], block_ref[0, 0, 3 - i]) for i in range(2)]
    top = pick(odd, top_ref, got_top_ref, 0)
    g = (near + lower(down_ref[0, 2, 0], top, down_ref[0, 2, 1])).astype(BF16)
    copies = []
    for i in range(2):
        gb = (nears[i] + lower(down_ref[0, i, 0], g, down_ref[0, i, 1])).astype(BF16)
        e = dot(outer_ref[i, 0], gb).astype(BF16)
        out[i] = (dense_ref[i] + contract(e, outer_ref[i, 1], 1, 1)).astype(BF16)
        copies.append(pltpu.make_async_copy(out.at[i], out_hbm.at[i], sems.at[i]))
        copies[-1].start()
    for copy in copies:
        copy.wait()


def in_vmem(n, scalar=True):
    specs = [pl.BlockSpec(memory_space=VMEM)] * n
    return [pl.BlockSpec(memory_space=pltpu.SMEM)] + specs if scalar else specs


def small(mib=2):
    return pltpu.CompilerParams(vmem_limit_bytes=mib << 20)


def exchange(block, b, count, keep=lambda p: True):
    route = [(p, p ^ (1 << b)) for p in range(count) if keep(p)]
    return lax.ppermute(block, AXES, route)


def stages(dense_a, dense_b, inner_basis_stack, outer_basis_stack, ascent, descent, couplings):
    count = lax.axis_size("row") * lax.axis_size("col")
    levels = count.bit_length() - 1
    rank = ascent.shape[-1]
    place = lax.axis_index(AXES).reshape(1).astype(jnp.int32)

    def mats(n):
        return jax.ShapeDtypeStruct((n, rank, rank), BF16)

    def odd(p):
        return p & 1 == 1

    swk, leaf_inner, pair = pl.pallas_call(
        head_kernel,
        out_shape=(mats(6), mats(2), mats(4)),
        in_specs=[pl.BlockSpec(memory_space=pltpu.HBM)] * 4,
        out_specs=tuple(in_vmem(3, False)),
        scratch_shapes=[
            VMEM(inner_basis_stack.shape, BF16),
            VMEM((3, 2, rank, rank), BF16),
            pltpu.SemaphoreType.DMA((5,)),
        ],
        compiler_params=small(4),
        cost_estimate=pl.CostEstimate(flops=1 << 28, bytes_accessed=0, transcendentals=0),
        name="head",
    )(inner_basis_stack, ascent, descent, couplings)

    carries, gots = [swk], []
    for b in range(levels):
        carry = carries[b]
        if b == 0:
            keep = lambda p: not odd(p)
        elif b == levels - 1:
            keep = lambda p: odd(p) and not (p >> b) & 1
        else:
            keep = odd
        got = exchange(carry, b, count, keep)
        gots.append(got)
        if b + 1 == levels:
            break
        if b == 0:
            carries.append(swk)
            continue
        carries.append(
            pl.pallas_call(
                functools.partial(carry_kernel, b),
                out_shape=mats(6 if b + 1 <= levels - 3 else 4),
                in_specs=in_vmem(2),
                out_specs=in_vmem(1, False)[0],
                compiler_params=small(),
                name="carry",
            )(place, carry, got)
        )

    dense = pl.pallas_call(
        dense_kernel,
        out_shape=jax.ShapeDtypeStruct(dense_a.shape, F32),
        in_specs=in_vmem(2, False),
        out_specs=in_vmem(1, False)[0],
        compiler_params=small(8),
        name="dense",
    )(dense_a, dense_b)

    received = []
    for b in range(levels):
        received.append(exchange(pair, b, count, odd if b else lambda p: True))
        if b + 1 < levels:
            out = 1 if b + 1 == levels - 1 else 2 if b + 1 == levels - 2 else 4
            pair = pl.pallas_call(
                functools.partial(round_kernel, b),
                out_shape=mats(out),
                in_specs=in_vmem(2),
                out_specs=in_vmem(1, False)[0],
                compiler_params=small(),
                name="round",
            )(place, pair, received[b])

    blocks = [block for both in zip(carries, gots) for block in both]
    top = pl.pallas_call(
        functools.partial(upper_kernel, levels),
        out_shape=mats(1),
        in_specs=in_vmem(levels - 1 + 2 * levels),
        out_specs=in_vmem(1, False)[0],
        compiler_params=small(4),
        name="upper",
    )(place, *received[1:], *blocks)
    got_top = exchange(top, 0, count, odd)

    return pl.pallas_call(
        final_kernel,
        out_shape=jax.ShapeDtypeStruct(dense.shape, BF16),
        in_specs=in_vmem(10),
        out_specs=pl.BlockSpec(memory_space=pltpu.HBM),
        scratch_shapes=[VMEM(dense.shape, BF16), pltpu.SemaphoreType.DMA((2,))],
        compiler_params=small(12),
        name="final",
    )(
        place,
        top,
        got_top,
        received[0],
        carries[0],
        gots[0],
        leaf_inner,
        descent,
        couplings,
        dense,
        outer_basis_stack,
    )


def solution(mesh):
    placed = (
        P(AXES, None, None),
        P(AXES, None, None),
        P(AXES, None, None, None),
        P(AXES, None, None, None),
        P(AXES, None, None, None, None),
        P(AXES, None, None, None, None),
        P(AXES, None, None, None, None),
    )
    return jax.shard_map(
        stages, mesh=mesh, in_specs=placed, out_specs=P(AXES, None, None), check_vma=False
    )
```

```python
import functools

import jax
import jax.numpy as jnp
from jax import lax
from jax.experimental import pallas as pl
from jax.experimental.pallas import tpu as pltpu
from jax.sharding import PartitionSpec as P

AXES = ("row", "col")
BF16 = jnp.bfloat16
F32 = jnp.float32
VMEM = pltpu.VMEM


def contract(a, b, left, right):
    return lax.dot_general(a, b, (((left,), (right,)), ((), ())), preferred_element_type=F32)


def dot(a, b):
    return contract(a, b, 1, 0)


def lift(p, f, q):
    return dot(contract(p, f, 0, 0).astype(BF16), q)


def couple(k, f, k2):
    return dot(dot(k, f).astype(BF16), k2)


def lower(s, g, w):
    return contract(dot(s, g).astype(BF16), w, 1, 1)


def pick(first, first_ref, second_ref, i):
    return jnp.where(first, first_ref[i], second_ref[i])


def head_kernel(inner_hbm, up_hbm, down_hbm, block_hbm, send_ref, leaf_ref, inner, up, sems):
    copies = [
        pltpu.make_async_copy(inner_hbm, inner, sems.at[0]),
        pltpu.make_async_copy(up_hbm.at[0, 0:3], up, sems.at[1]),
        pltpu.make_async_copy(up_hbm.at[0, 3], send_ref.at[2:4], sems.at[2]),
        pltpu.make_async_copy(down_hbm.at[0, 3], send_ref.at[4:6], sems.at[3]),
        pltpu.make_async_copy(block_hbm.at[0, 1], send_ref.at[6:10], sems.at[4]),
    ]
    for copy in copies:
        copy.start()
    copies[0].wait()
    leaves = [contract(inner[i, 0], inner[i, 1], 0, 0).astype(BF16) for i in range(2)]
    copies[1].wait()
    total = None
    for i in range(2):
        leaf_ref[i] = leaves[i]
        t = lift(up[i, 0], leaves[i], up[i, 1])
        total = t if total is None else total + t
    f0 = total.astype(BF16)
    send_ref[0] = f0
    send_ref[1] = lift(up[2, 0], f0, up[2, 1]).astype(BF16)
    for copy in copies[2:]:
        copy.wait()


def climb(low, r, levels, send_ref, got_ref, out_ref):
    f = (send_ref[1].astype(F32) + got_ref[1].astype(F32)).astype(BF16)
    out_ref[0] = f
    if r + 1 < levels - 1:
        p = pick(low, send_ref, got_ref, 2)
        q = pick(low, send_ref, got_ref, 3)
        out_ref[1] = lift(p, f, q).astype(BF16)
    if r + 1 < levels - 2:
        out_ref[2] = pick(low, got_ref, send_ref, 2)
        out_ref[3] = pick(low, got_ref, send_ref, 3)


def start_kernel(levels, position_ref, send_ref, got_ref, out_ref, carry_ref):
    odd = (position_ref[0] & 1) == 1

    @pl.when(odd)
    def _():
        climb(False, 0, levels, send_ref, got_ref, out_ref)

    @pl.when(jnp.logical_not(odd))
    def _():
        carry_ref[...] = got_ref[4:10]
        out_ref[0:2] = got_ref[7:9]


def sent(j, levels):
    return 6 if j <= levels - 4 else 4 if j == levels - 3 else 2


def fill(j, levels, position, carry_ref, out_ref):
    low = ((position >> j) & 1) == 0
    n = sent(j, levels)
    if n == 6:
        out_ref[0:6] = carry_ref[...]
        return

    @pl.when(low)
    def _():
        if n == 4:
            out_ref[0:2] = carry_ref[0:2]
        out_ref[n - 2 : n] = carry_ref[n - 1 : n + 1]

    @pl.when(jnp.logical_not(low))
    def _():
        out_ref[0:n] = carry_ref[2:6] if n == 4 else carry_ref[0:2]


def round_kernel(r, levels, position_ref, send_ref, got_ref, carry_ref, *out_refs):
    position = position_ref[0]
    odd = (position & 1) == 1
    out_ref = out_refs[0]

    @pl.when(odd)
    def _():
        low = ((position >> r) & 1) == 0
        if r == levels - 1:
            out_ref[0] = got_ref[0]
        else:
            climb(low, r, levels, send_ref, got_ref, out_ref)

    @pl.when(jnp.logical_not(odd))
    def _():
        if r == 1:
            new_ref = out_refs[1]
            mask = (1 << (levels - 2)) - 1
            top = ((position >> 1) & mask) == mask
            new_ref[...] = carry_ref[...]

            @pl.when(top)
            def _():
                left = ((position >> (levels - 1)) & 1) == 0
                new_ref[2] = pick(left, carry_ref.at[2:3], got_ref.at[0:1], 0)
                new_ref[3] = pick(left, carry_ref.at[5:6], got_ref.at[1:2], 0)

            fill(1, levels, position, new_ref, out_ref)
            return
        j = r - 1
        n = sent(j, levels)
        low = ((position >> j) & 1) == 0
        if n == 2:
            out_ref[0] = pick(low, carry_ref.at[0:1], got_ref.at[0:1], 0)
            out_ref[1] = pick(low, carry_ref.at[3:4], got_ref.at[1:2], 0)
            out_ref[2] = pick(low, got_ref.at[0:1], carry_ref.at[0:1], 0)
            out_ref[3] = pick(low, got_ref.at[1:2], carry_ref.at[1:2], 0)
            return
        new_ref, node_ref = out_refs[1:]

        @pl.when(low)
        def _():
            node_ref[0:3] = carry_ref[0:3]
            node_ref[3] = carry_ref[5]
            new_ref[...] = got_ref[0 : new_ref.shape[0]]

        @pl.when(jnp.logical_not(low))
        def _():
            node_ref[0:2] = got_ref[0:2]
            node_ref[2:4] = got_ref[3:5] if n == 6 else got_ref[2:4]
            new_ref[...] = carry_ref[...] if n == 6 else carry_ref[2:6]

        fill(j + 1, levels, position, new_ref, out_ref)


def pack_kernel(count, position_ref, *refs):
    odd = (position_ref[0] & 1) == 1
    received, nodes, out_ref = refs[:count], refs[count:-1], refs[-1]

    @pl.when(odd)
    def _():
        for i, ref in enumerate(received):
            out_ref[i] = ref[0]

    @pl.when(jnp.logical_not(odd))
    def _():
        for i, ref in enumerate(nodes):
            out_ref[4 * i : 4 * i + 4] = ref[...]


def dense_kernel(a_ref, b_ref, o_ref):
    for i in range(2):
        o_ref[i] = dot(a_ref[i], b_ref[i])


def final_kernel(
    levels, position_ref, send_ref, got_ref, mine_ref, other_ref, last_ref, other_last_ref,
    leaf_ref, down_ref, block_ref, dense_ref, outer_ref, out_hbm, out, sems,
):
    odd = (position_ref[0] & 1) == 1

    def inner(height):
        if height == levels - 1:
            return pick(odd, last_ref, other_last_ref, 0)
        return pick(odd, mine_ref, other_ref, height - 1)

    def generator(height, i):
        if height == 1:
            left, right = ((4, 4), (5, 5), (6, 7), (9, 8))[i]
            return jnp.where(odd, got_ref[right], send_ref[left])
        if height >= levels - 1:
            return pick(odd, other_last_ref, last_ref, 2 * (height - levels + 1) + i - 2)
        return pick(odd, other_ref, mine_ref, 4 * (height - 2) + i)

    coupling = None
    for height in range(levels, 1, -1):
        near = couple(generator(height, 2), inner(height - 1), generator(height, 3))
        if coupling is not None:
            near = near + lower(generator(height - 1, 0), coupling, generator(height - 1, 1))
        coupling = near.astype(BF16)
    near = couple(generator(1, 2), got_ref[0], generator(1, 3))
    g = (near + lower(down_ref[0, 2, 0], coupling, down_ref[0, 2, 1])).astype(BF16)
    copies = []
    for i in range(2):
        near = couple(block_ref[0, 0, i], leaf_ref[1 - i], block_ref[0, 0, 3 - i])
        gb = (near + lower(down_ref[0, i, 0], g, down_ref[0, i, 1])).astype(BF16)
        e = dot(outer_ref[i, 0], gb).astype(BF16)
        out[i] = (dense_ref[i] + contract(e, outer_ref[i, 1], 1, 1)).astype(BF16)
        copies.append(pltpu.make_async_copy(out.at[i], out_hbm.at[i], sems.at[i]))
        copies[-1].start()
    for copy in copies:
        copy.wait()


def in_vmem(n, scalar=True):
    specs = [pl.BlockSpec(memory_space=VMEM)] * n
    return [pl.BlockSpec(memory_space=pltpu.SMEM)] + specs if scalar else specs


def small(mib=2):
    return pltpu.CompilerParams(vmem_limit_bytes=mib << 20)


def exchange(block, count, odd_bit, even_bit):
    route = [(p, p ^ (1 << (odd_bit if p & 1 else even_bit))) for p in range(count)]
    return lax.ppermute(block, AXES, route)


def stages(dense_a, dense_b, inner_basis_stack, outer_basis_stack, ascent, descent, couplings):
    count = lax.axis_size("row") * lax.axis_size("col")
    levels = count.bit_length() - 1
    rank = ascent.shape[-1]
    place = lax.axis_index(AXES).reshape(1).astype(jnp.int32)

    def mats(n):
        return jax.ShapeDtypeStruct((n, rank, rank), BF16)

    def call(kernel, outs, *refs, **extra):
        return pl.pallas_call(
            kernel,
            out_shape=tuple(mats(n) for n in outs),
            in_specs=in_vmem(len(refs)),
            out_specs=tuple(in_vmem(len(outs), False)),
            compiler_params=small(),
        )(place, *refs)

    send, leaf_inner = pl.pallas_call(
        head_kernel,
        out_shape=(mats(10), mats(2)),
        in_specs=[pl.BlockSpec(memory_space=pltpu.HBM)] * 4,
        out_specs=tuple(in_vmem(2, False)),
        scratch_shapes=[
            VMEM(inner_basis_stack.shape, BF16),
            VMEM((3, 2, rank, rank), BF16),
            pltpu.SemaphoreType.DMA((5,)),
        ],
        compiler_params=small(4),
        name="head",
    )(*[
        pltpu.with_memory_space_constraint(x, pltpu.HBM)
        for x in (inner_basis_stack, ascent, descent, couplings)
    ])
    dense = pl.pallas_call(
        dense_kernel,
        out_shape=jax.ShapeDtypeStruct(dense_a.shape, F32),
        in_specs=in_vmem(2, False),
        out_specs=in_vmem(1, False)[0],
        compiler_params=small(8),
        name="dense",
    )(dense_a, dense_b)

    def width(r):
        climbing = 4 if r <= levels - 3 else 2 if r == levels - 2 else 1
        return max(climbing, 2 if r == 1 else sent(r - 1, levels))

    got = exchange(send, count, 0, 0)
    block, carry = call(functools.partial(start_kernel, levels), (width(1), 6), send, got)
    received, nodes = [], []
    for r in range(1, levels):
        new = exchange(block, count, r, levels - 1 if r == 1 else r - 1)
        kernel = functools.partial(round_kernel, r, levels)
        if r == levels - 1:
            (last,) = call(kernel, (4,), block, new, carry)
            break
        received.append(new)
        outs = (width(r + 1), 6 if r <= levels - 3 else 4) + ((4,) if r > 1 else ())
        block, carry, *node = call(kernel, outs, block, new, carry)
        nodes += node

    size = max(len(received), 4 * len(nodes))
    (mine,) = call(functools.partial(pack_kernel, len(received)), (size,), *received, *nodes)
    other = exchange(mine, count, 0, 0)
    other_last = exchange(last, count, 0, 0)

    return pl.pallas_call(
        functools.partial(final_kernel, levels),
        out_shape=jax.ShapeDtypeStruct(dense.shape, BF16),
        in_specs=in_vmem(11),
        out_specs=pl.BlockSpec(memory_space=pltpu.HBM),
        scratch_shapes=[VMEM(dense.shape, BF16), pltpu.SemaphoreType.DMA((2,))],
        compiler_params=small(12),
        name="final",
    )(
        place,
        send,
        got,
        mine,
        other,
        last,
        other_last,
        leaf_inner,
        descent,
        couplings,
        dense,
        outer_basis_stack,
    )


def solution(mesh):
    placed = (
        P(AXES, None, None),
        P(AXES, None, None),
        P(AXES, None, None, None),
        P(AXES, None, None, None),
        P(AXES, None, None, None, None),
        P(AXES, None, None, None, None),
        P(AXES, None, None, None, None),
    )
    return jax.shard_map(
        stages, mesh=mesh, in_specs=placed, out_specs=P(AXES, None, None), check_vma=False
    )
```

```python
import functools

import jax
import jax.numpy as jnp
from jax import lax
from jax.experimental import pallas as pl
from jax.experimental.pallas import tpu as pltpu
from jax.sharding import PartitionSpec as P

AXES = ("row", "col")
BF16 = jnp.bfloat16
F32 = jnp.float32
VMEM = pltpu.VMEM


def contract(a, b, left, right):
    return lax.dot_general(a, b, (((left,), (right,)), ((), ())), preferred_element_type=F32)


def dot(a, b):
    return contract(a, b, 1, 0)


def lift(p, f, q):
    return dot(contract(p, f, 0, 0).astype(BF16), q)


def couple(k, f, k2):
    return dot(dot(k, f).astype(BF16), k2)


def lower(s, g, w):
    return contract(dot(s, g).astype(BF16), w, 1, 1)


def pick(first, first_ref, second_ref, i):
    return jnp.where(first, first_ref[i], second_ref[i])


def head_kernel(inner_hbm, up_hbm, down_hbm, block_hbm, send_ref, leaf_ref, inner, up, sems):
    copies = [
        pltpu.make_async_copy(inner_hbm, inner, sems.at[0]),
        pltpu.make_async_copy(up_hbm.at[0, 0:3], up, sems.at[1]),
        pltpu.make_async_copy(up_hbm.at[0, 3], send_ref.at[2:4], sems.at[2]),
        pltpu.make_async_copy(down_hbm.at[0, 3], send_ref.at[4:6], sems.at[3]),
        pltpu.make_async_copy(block_hbm.at[0, 1], send_ref.at[6:10], sems.at[4]),
    ]
    for copy in copies:
        copy.start()
    copies[0].wait()
    leaves = [contract(inner[i, 0], inner[i, 1], 0, 0).astype(BF16) for i in range(2)]
    copies[1].wait()
    total = None
    for i in range(2):
        leaf_ref[i] = leaves[i]
        t = lift(up[i, 0], leaves[i], up[i, 1])
        total = t if total is None else total + t
    f0 = total.astype(BF16)
    send_ref[0] = f0
    send_ref[1] = lift(up[2, 0], f0, up[2, 1]).astype(BF16)
    for copy in copies[2:]:
        copy.wait()


def climb(low, r, levels, send_ref, got_ref, out_ref):
    f = (send_ref[1].astype(F32) + got_ref[1].astype(F32)).astype(BF16)
    out_ref[0] = f
    if r + 1 < levels - 1:
        p = pick(low, send_ref, got_ref, 2)
        q = pick(low, send_ref, got_ref, 3)
        out_ref[1] = lift(p, f, q).astype(BF16)
        out_ref[2] = pick(low, got_ref, send_ref, 2)
        out_ref[3] = pick(low, got_ref, send_ref, 3)


def start_kernel(levels, position_ref, send_ref, got_ref, out_ref, carry_ref):
    position = position_ref[0]
    odd = (position & 1) == 1
    high = ((position >> (levels - 2)) & 1) == 1

    @pl.when(odd)
    def _():
        climb(False, 0, levels, send_ref, got_ref, out_ref)

    @pl.when(position == (1 << (levels - 1)) - 1)
    def _():
        out_ref[2:4] = send_ref[7:9]

    @pl.when(jnp.logical_not(odd))
    def _():
        carry_ref[...] = got_ref[4:10]
        out_ref[0] = jnp.where(high, got_ref[6], got_ref[7])
        out_ref[1] = jnp.where(high, got_ref[9], got_ref[8])


def sent(j, levels):
    return 6 if j <= levels - 4 else 4


def fill(j, levels, position, carry_ref, out_ref):
    if sent(j, levels) == 6:
        out_ref[0:6] = carry_ref[...]
        return
    low = ((position >> j) & 1) == 0

    @pl.when(low)
    def _():
        out_ref[0:2] = carry_ref[0:2]
        out_ref[2:4] = carry_ref[3:5]

    @pl.when(jnp.logical_not(low))
    def _():
        out_ref[0:4] = carry_ref[2:6]


def round_kernel(r, levels, position_ref, send_ref, got_ref, carry_ref, out_ref, new_ref, *node_refs):
    position = position_ref[0]
    odd = (position & 1) == 1

    @pl.when(odd)
    def _():
        low = ((position >> r) & 1) == 0
        climb(low, r, levels, send_ref, got_ref, out_ref)
        if r == levels - 2:
            @pl.when(((position >> (levels - 1)) & 1) == 0)
            def _():
                k1 = pick(low, got_ref, send_ref, 2)
                k2 = pick(low, got_ref, send_ref, 3)
                out_ref[0] = couple(k1, out_ref[0], k2).astype(BF16)

    @pl.when(jnp.logical_not(odd))
    def _():
        if r == 1:
            mask = (1 << (levels - 3)) - 1
            top = ((position >> 1) & mask) == mask
            new_ref[...] = carry_ref[...]

            @pl.when(top)
            def _():
                low = ((position >> (levels - 2)) & 1) == 0
                for i, own in ((0, 2), (1, 5)):
                    new_ref[2 + i] = jnp.where(low, carry_ref[own], got_ref[i])
                    new_ref[4 + i] = jnp.where(low, got_ref[i], carry_ref[own])

            fill(1, levels, position, new_ref, out_ref)
            return
        j = r - 1
        (node_ref,) = node_refs
        low = ((position >> j) & 1) == 0
        full = sent(j, levels) == 6

        @pl.when(low)
        def _():
            node_ref[0:3] = carry_ref[0:3]
            node_ref[3] = carry_ref[5]
            new_ref[...] = got_ref[0 : new_ref.shape[0]]

        @pl.when(jnp.logical_not(low))
        def _():
            node_ref[0:2] = got_ref[0:2]
            node_ref[2:4] = got_ref[3:5] if full else got_ref[2:4]
            new_ref[...] = carry_ref[...] if full else carry_ref[2:6]

        if full:
            fill(j + 1, levels, position, new_ref, out_ref)


def pack_kernel(count, position_ref, *refs):
    odd = (position_ref[0] & 1) == 1
    received, nodes, top_ref, out_ref = refs[:count], refs[count:-2], refs[-2], refs[-1]

    @pl.when(odd)
    def _():
        for i, ref in enumerate(received):
            out_ref[i] = ref[0]

    @pl.when(jnp.logical_not(odd))
    def _():
        for i, ref in enumerate(nodes):
            out_ref[4 * i : 4 * i + 4] = ref[...]
        out_ref[4 * len(nodes) : 4 * len(nodes) + 4] = top_ref[...]


def dense_kernel(a_ref, b_ref, o_ref):
    for i in range(2):
        o_ref[i] = dot(a_ref[i], b_ref[i])


def first_node(odd, send_ref, got_ref, i):
    left, right = ((4, 4), (5, 5), (6, 7), (9, 8))[i]
    return jnp.where(odd, got_ref[right], send_ref[left])


def prepare_kernel(
    position_ref, send_ref, got_ref, leaf_ref, down_ref, block_ref, base_ref, left_ref, right_ref
):
    odd = (position_ref[0] & 1) == 1
    near = couple(
        first_node(odd, send_ref, got_ref, 2), got_ref[0], first_node(odd, send_ref, got_ref, 3)
    ).astype(BF16)
    for i in range(2):
        s, w = down_ref[0, i, 0], down_ref[0, i, 1]
        leaf = couple(block_ref[0, 0, i], leaf_ref[1 - i], block_ref[0, 0, 3 - i])
        base_ref[i] = leaf + lower(s, near, w)
        left_ref[i] = dot(s, down_ref[0, 2, 0]).astype(BF16)
        right_ref[i] = contract(down_ref[0, 2, 1], w, 0, 1).astype(BF16)


def upper_kernel(
    levels, position_ref, send_ref, got_ref, mine_ref, other_ref, base_ref, left_ref, right_ref
):
    position = position_ref[0]
    odd = (position & 1) == 1
    in_left = ((position >> (levels - 1)) & 1) == 0

    def inner(height):
        return pick(odd, mine_ref, other_ref, height - 1)

    def generator(height, i):
        if height == 1:
            return first_node(odd, send_ref, got_ref, i)
        slot = 4 * (height - 2) + i
        if height >= levels - 1:
            slot = 4 * (levels - 3) + 2 * (height - levels + 1) + i - 2
        return pick(odd, other_ref, mine_ref, slot)

    base = None
    left, right = generator(levels, 2), generator(levels, 3)
    for height in range(levels - 1, 1, -1):
        near = couple(generator(height, 2), inner(height - 1), generator(height, 3))
        s, w = generator(height - 1, 0), generator(height - 1, 1)
        if base is None:
            left = jnp.where(in_left, dot(s, left), s.astype(F32)).astype(BF16)
            right = jnp.where(in_left, contract(right, w, 1, 1), w.astype(F32).T).astype(BF16)
        else:
            left = dot(s, left).astype(BF16)
            right = contract(right, w, 1, 1).astype(BF16)
        base = near if base is None else near + lower(s, base.astype(BF16), w)
    base_ref[0] = base
    left_ref[0] = left
    right_ref[0] = right


def final_kernel(
    position_ref, last_ref, other_last_ref, base_ref, left_ref, right_ref, leaf_base_ref,
    leaf_left_ref, leaf_right_ref, dense_ref, outer_ref, out_hbm, out, sems,
):
    odd = (position_ref[0] & 1) == 1
    f = pick(odd, last_ref, other_last_ref, 0)
    g = (base_ref[0] + couple(left_ref[0], f, right_ref[0])).astype(BF16)
    copies = []
    for i in range(2):
        gb = leaf_base_ref[i] + couple(leaf_left_ref[i], g, leaf_right_ref[i])
        e = dot(outer_ref[i, 0], gb.astype(BF16)).astype(BF16)
        out[i] = (dense_ref[i] + contract(e, outer_ref[i, 1], 1, 1)).astype(BF16)
        copies.append(pltpu.make_async_copy(out.at[i], out_hbm.at[i], sems.at[i]))
        copies[-1].start()
    for copy in copies:
        copy.wait()


def in_vmem(n, scalar=True):
    specs = [pl.BlockSpec(memory_space=VMEM)] * n
    return [pl.BlockSpec(memory_space=pltpu.SMEM)] + specs if scalar else specs


def small(mib=2):
    return pltpu.CompilerParams(vmem_limit_bytes=mib << 20)


def exchange(block, count, odd_bit, even_bit):
    route = [(p, p ^ (1 << (odd_bit if p & 1 else even_bit))) for p in range(count)]
    return lax.ppermute(block, AXES, route)


def stages(dense_a, dense_b, inner_basis_stack, outer_basis_stack, ascent, descent, couplings):
    count = lax.axis_size("row") * lax.axis_size("col")
    levels = count.bit_length() - 1
    rank = ascent.shape[-1]
    place = lax.axis_index(AXES).reshape(1).astype(jnp.int32)

    def mats(n, dtype=BF16):
        return jax.ShapeDtypeStruct((n, rank, rank), dtype)

    def call(kernel, outs, *refs, **extra):
        return pl.pallas_call(
            kernel,
            out_shape=tuple(mats(n) if n > 0 else mats(-n, F32) for n in outs),
            in_specs=in_vmem(len(refs)),
            out_specs=tuple(in_vmem(len(outs), False)),
            compiler_params=small(),
        )(place, *refs)

    send, leaf_inner = pl.pallas_call(
        head_kernel,
        out_shape=(mats(10), mats(2)),
        in_specs=[pl.BlockSpec(memory_space=pltpu.HBM)] * 4,
        out_specs=tuple(in_vmem(2, False)),
        scratch_shapes=[
            VMEM(inner_basis_stack.shape, BF16),
            VMEM((3, 2, rank, rank), BF16),
            pltpu.SemaphoreType.DMA((5,)),
        ],
        compiler_params=small(4),
        name="head",
    )(*[
        pltpu.with_memory_space_constraint(x, pltpu.HBM)
        for x in (inner_basis_stack, ascent, descent, couplings)
    ])
    dense = pl.pallas_call(
        dense_kernel,
        out_shape=jax.ShapeDtypeStruct(dense_a.shape, F32),
        in_specs=in_vmem(2, False),
        out_specs=in_vmem(1, False)[0],
        compiler_params=small(8),
        name="dense",
    )(dense_a, dense_b)

    def width(r):
        climbing = 4 if r <= levels - 2 else 1
        return climbing if r in (1, levels - 1) else max(climbing, sent(r - 1, levels))

    got = exchange(send, count, 0, 0)
    block, carry = call(functools.partial(start_kernel, levels), (width(1), 6), send, got)
    leaf_terms = call(prepare_kernel, (-2, 2, 2), send, got, leaf_inner, descent, couplings)
    received, nodes = [], []
    for r in range(1, levels - 1):
        new = exchange(block, count, r, levels - 2 if r == 1 else r - 1)
        received.append(new)
        outs = (width(r + 1), 4 if r == levels - 2 else 6) + ((4,) if r > 1 else ())
        kernel = functools.partial(round_kernel, r, levels)
        block, carry, *node = call(kernel, outs, block, new, carry)
        nodes += node
    last = exchange(block, count, levels - 1, 1)

    size = 4 * len(nodes) + 4
    kernel = functools.partial(pack_kernel, len(received))
    (mine,) = call(kernel, (size,), *received, *nodes, carry)
    other = exchange(mine, count, 0, 0)
    kernel = functools.partial(upper_kernel, levels)
    upper_terms = call(kernel, (-1, 1, 1), send, got, mine, other)
    other_last = exchange(last, count, 0, 0)

    return pl.pallas_call(
        final_kernel,
        out_shape=jax.ShapeDtypeStruct(dense.shape, BF16),
        in_specs=in_vmem(10),
        out_specs=pl.BlockSpec(memory_space=pltpu.HBM),
        scratch_shapes=[VMEM(dense.shape, BF16), pltpu.SemaphoreType.DMA((2,))],
        compiler_params=small(12),
        name="final",
    )(place, last, other_last, *upper_terms, *leaf_terms, dense, outer_basis_stack)


def solution(mesh):
    placed = (
        P(AXES, None, None),
        P(AXES, None, None),
        P(AXES, None, None, None),
        P(AXES, None, None, None),
        P(AXES, None, None, None, None),
        P(AXES, None, None, None, None),
        P(AXES, None, None, None, None),
    )
    return jax.shard_map(
        stages, mesh=mesh, in_specs=placed, out_specs=P(AXES, None, None), check_vma=False
    )
```

```python
import functools

import jax
import jax.numpy as jnp
from jax import lax
from jax.experimental import pallas as pl
from jax.experimental.pallas import tpu as pltpu
from jax.sharding import PartitionSpec as P

AXES = ("row", "col")
BF16 = jnp.bfloat16
F32 = jnp.float32
VMEM = pltpu.VMEM
CHUNKS = 2


def contract(a, b, left, right):
    return lax.dot_general(a, b, (((left,), (right,)), ((), ())), preferred_element_type=F32)


def dot(a, b):
    return contract(a, b, 1, 0)


def lift(p, f, q):
    return dot(contract(p, f, 0, 0).astype(BF16), q)


def couple(k, f, k2):
    return dot(dot(k, f).astype(BF16), k2)


def lower(s, g, w):
    return contract(dot(s, g).astype(BF16), w, 1, 1)


def pick(first, first_ref, second_ref, i):
    return jnp.where(first, first_ref[i], second_ref[i])


def head_kernel(
    levels, position_ref, inner_hbm, up_hbm, down_hbm, block_hbm,
    send_ref, pq_ref, swk_ref, leaf_ref, inner, up, sems,
):
    copies = [
        pltpu.make_async_copy(up_hbm.at[0, 0:3], up, sems.at[0]),
        pltpu.make_async_copy(inner_hbm.at[0], inner.at[0], sems.at[1]),
        pltpu.make_async_copy(inner_hbm.at[1], inner.at[1], sems.at[2]),
        pltpu.make_async_copy(up_hbm.at[0, 3], pq_ref, sems.at[3]),
        pltpu.make_async_copy(down_hbm.at[0, 3], swk_ref.at[0:2], sems.at[4]),
        pltpu.make_async_copy(block_hbm.at[0, 1], swk_ref.at[2:6], sems.at[5]),
    ]
    for copy in copies:
        copy.start()
    copies[0].wait()
    twice = [[dot(up[i, k], up[2, k]).astype(BF16) for k in range(2)] for i in range(2)]
    leaves = []
    for i in range(2):
        copies[1 + i].wait()
        leaves.append(contract(inner[i, 0], inner[i, 1], 0, 0).astype(BF16))
        leaf_ref[i] = leaves[i]
    halves = [
        (contract(up[i, 0], leaves[i], 0, 0).astype(BF16),
         contract(twice[i][0], leaves[i], 0, 0).astype(BF16))
        for i in range(2)
    ]
    f = [dot(halves[i][0], up[i, 1]) for i in range(2)]
    t = [dot(halves[i][1], twice[i][1]) for i in range(2)]
    send_ref[0] = (f[0] + f[1]).astype(BF16)
    send_ref[1] = (t[0] + t[1]).astype(BF16)
    for copy in copies[3:]:
        copy.wait()
    odd = (position_ref[0] & 1) == 1
    high = (position_ref[0] >> (levels - 2)) & 1
    send_ref[2] = jnp.where(odd, swk_ref[3 - high], pq_ref[0])
    send_ref[3] = jnp.where(odd, swk_ref[4 + high], pq_ref[1])


def climb(low, r, levels, send_ref, got_ref, out_ref):
    f = (send_ref[1].astype(F32) + got_ref[1].astype(F32)).astype(BF16)
    out_ref[0] = f
    if r + 1 < levels - 1:
        p = pick(low, send_ref, got_ref, 2)
        q = pick(low, send_ref, got_ref, 3)
        out_ref[1] = lift(p, f, q).astype(BF16)
        out_ref[2] = pick(low, got_ref, send_ref, 2)
        out_ref[3] = pick(low, got_ref, send_ref, 3)


def start_kernel(levels, position_ref, send_ref, got_ref, pq_ref, swk_ref, out_ref):
    position = position_ref[0]
    odd = (position & 1) == 1
    root = position == (1 << (levels - 1)) - 1

    @pl.when(odd)
    def _():
        f = (send_ref[1].astype(F32) + got_ref[1].astype(F32)).astype(BF16)
        out_ref[0] = f
        out_ref[1] = lift(got_ref[2], f, got_ref[3]).astype(BF16)
        out_ref[2] = jnp.where(root, swk_ref[3], pq_ref[0])
        out_ref[3] = jnp.where(root, swk_ref[4], pq_ref[1])

    @pl.when(jnp.logical_not(odd))
    def _():
        out_ref[0:2] = got_ref[2:4]


def sent(j, levels):
    return 6 if j <= levels - 4 else 4


def fill(j, levels, position, carry_ref, out_ref):
    if sent(j, levels) == 6:
        out_ref[0:6] = carry_ref[...]
        return
    low = ((position >> j) & 1) == 0

    @pl.when(low)
    def _():
        out_ref[0:2] = carry_ref[0:2]
        out_ref[2:4] = carry_ref[3:5]

    @pl.when(jnp.logical_not(low))
    def _():
        out_ref[0:4] = carry_ref[2:6]


def round_kernel(r, levels, position_ref, send_ref, got_ref, carry_ref, out_ref, new_ref, *node_refs):
    position = position_ref[0]
    odd = (position & 1) == 1

    @pl.when(odd)
    def _():
        low = ((position >> r) & 1) == 0
        climb(low, r, levels, send_ref, got_ref, out_ref)
        if r == levels - 2:
            @pl.when(((position >> (levels - 1)) & 1) == 0)
            def _():
                k1 = pick(low, got_ref, send_ref, 2)
                k2 = pick(low, got_ref, send_ref, 3)
                out_ref[0] = couple(k1, out_ref[0], k2).astype(BF16)

    @pl.when(jnp.logical_not(odd))
    def _():
        if r == 1:
            mask = (1 << (levels - 3)) - 1
            top = ((position >> 1) & mask) == mask
            new_ref[...] = carry_ref[...]

            @pl.when(top)
            def _():
                low = ((position >> (levels - 2)) & 1) == 0
                for i, own in ((0, 2), (1, 5)):
                    new_ref[2 + i] = jnp.where(low, carry_ref[own], got_ref[i])
                    new_ref[4 + i] = jnp.where(low, got_ref[i], carry_ref[own])

            fill(1, levels, position, new_ref, out_ref)
            return
        j = r - 1
        (node_ref,) = node_refs
        low = ((position >> j) & 1) == 0
        full = sent(j, levels) == 6

        @pl.when(low)
        def _():
            node_ref[0:3] = carry_ref[0:3]
            node_ref[3] = carry_ref[5]
            new_ref[...] = got_ref[0 : new_ref.shape[0]]

        @pl.when(jnp.logical_not(low))
        def _():
            node_ref[0:2] = got_ref[0:2]
            node_ref[2:4] = got_ref[3:5] if full else got_ref[2:4]
            new_ref[...] = carry_ref[...] if full else carry_ref[2:6]

        if full:
            fill(j + 1, levels, position, new_ref, out_ref)


def pack_kernel(count, position_ref, *refs):
    odd = (position_ref[0] & 1) == 1
    received, nodes, top_ref, out_ref = refs[:count], refs[count:-2], refs[-2], refs[-1]

    @pl.when(odd)
    def _():
        for i, ref in enumerate(received):
            out_ref[i] = ref[0]

    @pl.when(jnp.logical_not(odd))
    def _():
        for i, ref in enumerate(nodes):
            out_ref[4 * i : 4 * i + 4] = ref[...]
        out_ref[4 * len(nodes) : 4 * len(nodes) + 4] = top_ref[...]


def dense_kernel(a_ref, b_ref, o_ref):
    for i in range(2):
        o_ref[i] = dot(a_ref[i], b_ref[i])


def first_node(odd, swk_ref, other_swk_ref, i):
    left, right = ((0, 0), (1, 1), (2, 3), (5, 4))[i]
    return jnp.where(odd, other_swk_ref[right], swk_ref[left])


def prepare_kernel(
    position_ref, got_ref, swk_ref, other_swk_ref, leaf_ref, down_ref, block_ref, dense_ref,
    outer_ref, out_ref, left_ref, right_ref,
):
    odd = (position_ref[0] & 1) == 1
    near = couple(
        first_node(odd, swk_ref, other_swk_ref, 2),
        got_ref[0],
        first_node(odd, swk_ref, other_swk_ref, 3),
    ).astype(BF16)
    for i in range(2):
        s, w = down_ref[0, i, 0], down_ref[0, i, 1]
        leaf = couple(block_ref[0, 0, i], leaf_ref[1 - i], block_ref[0, 0, 3 - i])
        g = (leaf + lower(s, near, w)).astype(BF16)
        e = dot(outer_ref[i, 0], g).astype(BF16)
        out_ref[i] = dense_ref[i] + contract(e, outer_ref[i, 1], 1, 1)
        left = dot(s, down_ref[0, 2, 0]).astype(BF16)
        right = dot(w, down_ref[0, 2, 1]).astype(BF16)
        left_ref[i] = dot(outer_ref[i, 0], left).astype(BF16)
        right_ref[i] = dot(outer_ref[i, 1], right).astype(BF16)


def upper_kernel(
    levels, position_ref, swk_ref, other_swk_ref, mine_ref, other_ref, base_ref, left_ref, right_ref
):
    position = position_ref[0]
    odd = (position & 1) == 1
    in_left = ((position >> (levels - 1)) & 1) == 0

    def inner(height):
        return pick(odd, mine_ref, other_ref, height - 1)

    def generator(height, i):
        if height == 1:
            return first_node(odd, swk_ref, other_swk_ref, i)
        slot = 4 * (height - 2) + i
        if height >= levels - 1:
            slot = 4 * (levels - 3) + 2 * (height - levels + 1) + i - 2
        return pick(odd, other_ref, mine_ref, slot)

    heights = range(2, levels)
    nears = [dot(generator(h, 2), inner(h - 1)).astype(BF16) for h in heights]
    sides = [(generator(1, 0), generator(1, 1))]
    for n, h in enumerate(heights):
        nears[n] = dot(nears[n], generator(h, 3))
        if h < levels - 1:
            s, w = (dot(x, generator(h, k)).astype(BF16) for k, x in enumerate(sides[-1]))
            sides.append((s, w))
    left, right = sides[-1]
    left_ref[0] = jnp.where(in_left, dot(left, generator(levels, 2)).astype(BF16), left)
    right_ref[0] = jnp.where(
        in_left, contract(right, generator(levels, 3), 1, 1).astype(BF16), right
    )
    base = nears[0]
    halves = [dot(s, near.astype(BF16)).astype(BF16) for (s, _), near in zip(sides, nears[1:])]
    for half, (_, w) in zip(halves, sides):
        base = base + contract(half, w, 1, 1)
    base_ref[0] = base.astype(BF16)


def merge_kernel(
    base_ref, left_ref, right_ref, leaf_left_ref, leaf_right_ref, out_left_ref, both_left_ref,
    both_right_ref,
):
    rank = base_ref.shape[-1]
    for i in range(2):
        both_left_ref[i] = dot(leaf_left_ref[i], base_ref[0]).astype(BF16)
        out_left_ref[i] = dot(leaf_left_ref[i], left_ref[0]).astype(BF16)
        both_right_ref[i, :, :rank] = dot(leaf_right_ref[i], right_ref[0]).astype(BF16)
        both_right_ref[i, :, rank:] = leaf_right_ref[i]


def final_kernel(
    position_ref, last_ref, other_last_ref, part_ref, left_ref, base_ref, right_ref, out_hbm, out,
    sems,
):
    odd = (position_ref[0] & 1) == 1
    f = pick(odd, last_ref, other_last_ref, 0)
    rows = part_ref.shape[1] // CHUNKS
    copies = []
    lasts = [dot(left_ref[i], f).astype(BF16) for i in range(2)]
    for i in range(2):
        e = jnp.concatenate([lasts[i], base_ref[i]], 1)
        for c in range(CHUNKS):
            here = pl.ds(c * rows, rows)
            full = part_ref[i, here] + contract(e[c * rows : (c + 1) * rows], right_ref[i], 1, 1)
            out[i, here] = full.astype(BF16)
            k = i * CHUNKS + c
            copies.append(pltpu.make_async_copy(out.at[i, here], out_hbm.at[i, here], sems.at[k]))
            copies[-1].start()
    for copy in copies:
        copy.wait()


def in_vmem(n, scalar=True):
    specs = [pl.BlockSpec(memory_space=VMEM)] * n
    return [pl.BlockSpec(memory_space=pltpu.SMEM)] + specs if scalar else specs


def small(mib=2):
    return pltpu.CompilerParams(vmem_limit_bytes=mib << 20)


def exchange(block, count, odd_bit, even_bit):
    route = [(p, p ^ (1 << (odd_bit if p & 1 else even_bit))) for p in range(count)]
    return lax.ppermute(block, AXES, route)


def stages(dense_a, dense_b, inner_basis_stack, outer_basis_stack, ascent, descent, couplings):
    count = lax.axis_size("row") * lax.axis_size("col")
    levels = count.bit_length() - 1
    rank = ascent.shape[-1]
    place = lax.axis_index(AXES).reshape(1).astype(jnp.int32)

    def mats(n):
        return jax.ShapeDtypeStruct((n, rank, rank), BF16)

    tall = jax.ShapeDtypeStruct(outer_basis_stack.shape[:1] + outer_basis_stack.shape[2:], BF16)

    wide = jax.ShapeDtypeStruct(tall.shape[:2] + (2 * rank,), BF16)
    whole = jax.ShapeDtypeStruct(dense_a.shape, F32)

    def call(kernel, outs, *refs, scalar=True, mib=2):
        outs = tuple(mats(n) if isinstance(n, int) else n for n in outs)
        return pl.pallas_call(
            kernel,
            out_shape=outs,
            in_specs=in_vmem(len(refs), scalar),
            out_specs=tuple(in_vmem(len(outs), False)),
            compiler_params=small(mib),
        )(*([place] if scalar else []), *refs)

    send, pq, swk, leaf_inner = pl.pallas_call(
        functools.partial(head_kernel, levels),
        out_shape=(mats(4), mats(2), mats(6), mats(2)),
        in_specs=[pl.BlockSpec(memory_space=pltpu.SMEM)]
        + [pl.BlockSpec(memory_space=pltpu.HBM)] * 4,
        out_specs=tuple(in_vmem(4, False)),
        scratch_shapes=[
            VMEM(inner_basis_stack.shape, BF16),
            VMEM((3, 2, rank, rank), BF16),
            pltpu.SemaphoreType.DMA((6,)),
        ],
        compiler_params=small(4),
        name="head",
    )(place, *[
        pltpu.with_memory_space_constraint(x, pltpu.HBM)
        for x in (inner_basis_stack, ascent, descent, couplings)
    ])
    dense = pl.pallas_call(
        dense_kernel,
        out_shape=jax.ShapeDtypeStruct(dense_a.shape, F32),
        in_specs=in_vmem(2, False),
        out_specs=in_vmem(1, False)[0],
        compiler_params=small(8),
        name="dense",
    )(dense_a, dense_b)

    def width(r):
        climbing = 4 if r <= levels - 2 else 1
        return climbing if r in (1, levels - 1) else max(climbing, sent(r - 1, levels))

    got = exchange(send, count, 0, 0)
    (block,) = call(functools.partial(start_kernel, levels), (width(1),), send, got, pq, swk)
    carry = other_swk = exchange(swk, count, 0, 0)
    part, *sides = call(
        prepare_kernel, (whole, tall, tall), got, swk, other_swk, leaf_inner,
        descent, couplings, dense, outer_basis_stack, mib=12,
    )
    received, nodes = [], []
    for r in range(1, levels - 1):
        new = exchange(block, count, r, levels - 2 if r == 1 else r - 1)
        received.append(new)
        outs = (width(r + 1), 4 if r == levels - 2 else 6) + ((4,) if r > 1 else ())
        kernel = functools.partial(round_kernel, r, levels)
        block, carry, *node = call(kernel, outs, block, new, carry)
        nodes += node
    last = exchange(block, count, levels - 1, 1)

    size = 4 * len(nodes) + 4
    kernel = functools.partial(pack_kernel, len(received))
    (mine,) = call(kernel, (size,), *received, *nodes, carry)
    other = exchange(mine, count, 0, 0)
    kernel = functools.partial(upper_kernel, levels)
    upper_terms = call(kernel, (1, 1, 1), swk, other_swk, mine, other)
    sides = call(merge_kernel, (tall, tall, wide), *upper_terms, *sides, scalar=False, mib=4)
    other_last = exchange(last, count, 0, 0)

    return pl.pallas_call(
        final_kernel,
        out_shape=jax.ShapeDtypeStruct(dense.shape, BF16),
        in_specs=in_vmem(6),
        out_specs=pl.BlockSpec(memory_space=pltpu.HBM),
        scratch_shapes=[VMEM(dense.shape, BF16), pltpu.SemaphoreType.DMA((2 * CHUNKS,))],
        compiler_params=small(12),
        name="final",
    )(place, last, other_last, part, *sides)


def solution(mesh):
    placed = (
        P(AXES, None, None),
        P(AXES, None, None),
        P(AXES, None, None, None),
        P(AXES, None, None, None),
        P(AXES, None, None, None, None),
        P(AXES, None, None, None, None),
        P(AXES, None, None, None, None),
    )
    return jax.shard_map(
        stages, mesh=mesh, in_specs=placed, out_specs=P(AXES, None, None), check_vma=False
    )
```

```python
import functools

import jax
import jax.numpy as jnp
from jax import lax
from jax.experimental import pallas as pl
from jax.experimental.pallas import tpu as pltpu
from jax.sharding import PartitionSpec as P

AXES = ("row", "col")
BF16 = jnp.bfloat16
F32 = jnp.float32
VMEM = pltpu.VMEM
CHUNKS = 2


def contract(a, b, left, right):
    return lax.dot_general(a, b, (((left,), (right,)), ((), ())), preferred_element_type=F32)


def dot(a, b):
    return contract(a, b, 1, 0)


def lift(p, f, q):
    return dot(contract(p, f, 0, 0).astype(BF16), q)


def couple(k, f, k2):
    return dot(dot(k, f).astype(BF16), k2)


def lower(s, g, w):
    return contract(dot(s, g).astype(BF16), w, 1, 1)


def pick(first, first_ref, second_ref, i):
    return jnp.where(first, first_ref[i], second_ref[i])


def head_kernel(
    levels, position_ref, inner_hbm, up_hbm, down_hbm, block_hbm,
    send_ref, pq_ref, swk_ref, leaf_ref, inner, up, sems,
):
    copies = [
        pltpu.make_async_copy(up_hbm.at[0, 0:3], up, sems.at[0]),
        pltpu.make_async_copy(inner_hbm.at[0], inner.at[0], sems.at[1]),
        pltpu.make_async_copy(inner_hbm.at[1], inner.at[1], sems.at[2]),
        pltpu.make_async_copy(up_hbm.at[0, 3], pq_ref, sems.at[3]),
        pltpu.make_async_copy(down_hbm.at[0, 3], swk_ref.at[0:2], sems.at[4]),
        pltpu.make_async_copy(block_hbm.at[0, 1], swk_ref.at[2:6], sems.at[5]),
    ]
    for copy in copies:
        copy.start()
    copies[0].wait()
    twice = [[dot(up[i, k], up[2, k]).astype(BF16) for k in range(2)] for i in range(2)]
    leaves = []
    for i in range(2):
        copies[1 + i].wait()
        leaves.append(contract(inner[i, 0], inner[i, 1], 0, 0).astype(BF16))
        leaf_ref[i] = leaves[i]
    halves = [
        (contract(up[i, 0], leaves[i], 0, 0).astype(BF16),
         contract(twice[i][0], leaves[i], 0, 0).astype(BF16))
        for i in range(2)
    ]
    f = [dot(halves[i][0], up[i, 1]) for i in range(2)]
    t = [dot(halves[i][1], twice[i][1]) for i in range(2)]
    send_ref[0] = (f[0] + f[1]).astype(BF16)
    send_ref[1] = (t[0] + t[1]).astype(BF16)
    for copy in copies[3:]:
        copy.wait()
    odd = (position_ref[0] & 1) == 1
    high = (position_ref[0] >> (levels - 2)) & 1
    send_ref[2] = jnp.where(odd, swk_ref[3 - high], pq_ref[0])
    send_ref[3] = jnp.where(odd, swk_ref[4 + high], pq_ref[1])


def climb(low, r, levels, send_ref, got_ref, out_ref):
    t = 0 if r == 1 else 1
    f = (send_ref[t].astype(F32) + got_ref[t].astype(F32)).astype(BF16)
    out_ref[0] = f
    if r + 1 < levels - 1:
        p = pick(low, send_ref, got_ref, t + 1)
        q = pick(low, send_ref, got_ref, t + 2)
        out_ref[1] = lift(p, f, q).astype(BF16)
        out_ref[2] = pick(low, got_ref, send_ref, t + 1)
        out_ref[3] = pick(low, got_ref, send_ref, t + 2)


def start_kernel(levels, position_ref, send_ref, got_ref, pq_ref, swk_ref, out_ref, f_ref):
    position = position_ref[0]
    odd = (position & 1) == 1
    root = position == (1 << (levels - 1)) - 1
    f = (send_ref[1].astype(F32) + got_ref[1].astype(F32)).astype(BF16)
    f_ref[0] = f

    @pl.when(odd)
    def _():
        out_ref[0] = lift(got_ref[2], f, got_ref[3]).astype(BF16)
        out_ref[1] = jnp.where(root, swk_ref[3], pq_ref[0])
        out_ref[2] = jnp.where(root, swk_ref[4], pq_ref[1])

    @pl.when(jnp.logical_not(odd))
    def _():
        out_ref[0:2] = got_ref[2:4]


def sent(j, levels):
    return 6 if j <= levels - 4 else 4


def fill(j, levels, position, carry_ref, out_ref):
    if sent(j, levels) == 6:
        out_ref[0:6] = carry_ref[...]
        return
    low = ((position >> j) & 1) == 0

    @pl.when(low)
    def _():
        out_ref[0:2] = carry_ref[0:2]
        out_ref[2:4] = carry_ref[3:5]

    @pl.when(jnp.logical_not(low))
    def _():
        out_ref[0:4] = carry_ref[2:6]


def round_kernel(r, levels, position_ref, send_ref, got_ref, carry_ref, *refs):
    if r == levels - 2:
        first_ref, out_ref, new_ref, *node_refs = refs
    else:
        out_ref, new_ref, *node_refs = refs
    position = position_ref[0]
    odd = (position & 1) == 1

    @pl.when(odd)
    def _():
        low = ((position >> r) & 1) == 0
        climb(low, r, levels, send_ref, got_ref, out_ref)
        if r == levels - 2:
            @pl.when(((position >> (levels - 1)) & 1) == 0)
            def _():
                k1 = pick(low, got_ref, send_ref, 2)
                k2 = pick(low, got_ref, send_ref, 3)
                out_ref[0] = couple(k1, out_ref[0], k2).astype(BF16)

    @pl.when(jnp.logical_not(odd))
    def _():
        if r == 1:
            mask = (1 << (levels - 3)) - 1
            top = ((position >> 1) & mask) == mask
            new_ref[...] = carry_ref[...]

            @pl.when(top)
            def _():
                low = ((position >> (levels - 2)) & 1) == 0
                for i, own in ((0, 2), (1, 5)):
                    new_ref[2 + i] = jnp.where(low, carry_ref[own], got_ref[i])
                    new_ref[4 + i] = jnp.where(low, got_ref[i], carry_ref[own])

            fill(1, levels, position, new_ref, out_ref)
            return
        j = r - 1
        (node_ref,) = node_refs
        low = ((position >> j) & 1) == 0
        full = sent(j, levels) == 6

        @pl.when(low)
        def _():
            node_ref[0:3] = carry_ref[0:3]
            node_ref[3] = carry_ref[5]
            new_ref[...] = got_ref[0 : new_ref.shape[0]]

        @pl.when(jnp.logical_not(low))
        def _():
            node_ref[0:2] = got_ref[0:2]
            node_ref[2:4] = got_ref[3:5] if full else got_ref[2:4]
            new_ref[...] = carry_ref[...] if full else carry_ref[2:6]

        if full:
            fill(j + 1, levels, position, new_ref, out_ref)
        if r == levels - 2:
            out_ref[0] = first_ref[0]


def pack_kernel(count, position_ref, *refs):
    odd = (position_ref[0] & 1) == 1
    received, nodes, top_ref, out_ref = refs[:count], refs[count:-2], refs[-2], refs[-1]

    @pl.when(odd)
    def _():
        for i, ref in enumerate(received):
            out_ref[i] = ref[0]

    @pl.when(jnp.logical_not(odd))
    def _():
        for i, ref in enumerate(nodes):
            out_ref[4 * i : 4 * i + 4] = ref[...]
        out_ref[4 * len(nodes) : 4 * len(nodes) + 4] = top_ref[...]


def dense_kernel(a_ref, b_ref, o_ref):
    for i in range(2):
        o_ref[i] = dot(a_ref[i], b_ref[i])


def first_node(odd, swk_ref, other_swk_ref, i):
    left, right = ((0, 0), (1, 1), (2, 3), (5, 4))[i]
    return jnp.where(odd, other_swk_ref[right], swk_ref[left])


def prepare_kernel(
    position_ref, got_ref, swk_ref, other_swk_ref, f_ref, leaf_ref, down_ref, block_ref, dense_ref,
    outer_ref, out_ref, left_ref, right_ref, first_ref, first_left_ref, first_right_ref,
):
    odd = (position_ref[0] & 1) == 1
    low = ((position_ref[0] >> 1) & 1) == 0
    node = [pick(odd, swk_ref, other_swk_ref, k) for k in range(2, 6)]
    first_ref[0] = jnp.where(low, couple(node[1], f_ref[0], node[2]).astype(BF16), f_ref[0])
    near = couple(
        first_node(odd, swk_ref, other_swk_ref, 2),
        got_ref[0],
        first_node(odd, swk_ref, other_swk_ref, 3),
    ).astype(BF16)
    for i in range(2):
        s, w = down_ref[0, i, 0], down_ref[0, i, 1]
        leaf = couple(block_ref[0, 0, i], leaf_ref[1 - i], block_ref[0, 0, 3 - i])
        g = (leaf + lower(s, near, w)).astype(BF16)
        e = dot(outer_ref[i, 0], g).astype(BF16)
        out_ref[i] = dense_ref[i] + contract(e, outer_ref[i, 1], 1, 1)
        left = dot(s, down_ref[0, 2, 0]).astype(BF16)
        right = dot(w, down_ref[0, 2, 1]).astype(BF16)
        left = dot(outer_ref[i, 0], left).astype(BF16)
        right = dot(outer_ref[i, 1], right).astype(BF16)
        left_ref[i] = left
        right_ref[i] = right
        first_left_ref[i] = jnp.where(low, dot(left, node[0]).astype(BF16), left)
        first_right_ref[i] = jnp.where(low, contract(right, node[3], 1, 1).astype(BF16), right)


def upper_kernel(
    levels, position_ref, swk_ref, other_swk_ref, mine_ref, other_ref, base_ref, left_ref, right_ref
):
    position = position_ref[0]
    odd = (position & 1) == 1
    in_left = ((position >> (levels - 1)) & 1) == 0

    def inner(height):
        return pick(odd, mine_ref, other_ref, height - 2)

    def generator(height, i):
        if height == 1:
            return first_node(odd, swk_ref, other_swk_ref, i)
        slot = 4 * (height - 2) + i
        if height >= levels - 1:
            slot = 4 * (levels - 3) + 2 * (height - levels + 1) + i - 2
        return pick(odd, other_ref, mine_ref, slot)

    heights = range(3, levels)
    nears = [dot(generator(h, 2), inner(h - 1)).astype(BF16) for h in heights]
    sides = [(generator(1, 0), generator(1, 1))]
    for n, h in enumerate(heights):
        nears[n] = dot(nears[n], generator(h, 3)).astype(BF16)
        s, w = (dot(x, generator(h - 1, k)).astype(BF16) for k, x in enumerate(sides[-1]))
        sides.append((s, w))
    left, right = sides[-1]
    left_ref[0] = jnp.where(in_left, dot(left, generator(levels, 2)).astype(BF16), left)
    right_ref[0] = jnp.where(
        in_left, contract(right, generator(levels, 3), 1, 1).astype(BF16), right
    )
    halves = [dot(s, near).astype(BF16) for (s, _), near in zip(sides, nears)]
    base = None
    for half, (_, w) in zip(halves, sides):
        term = contract(half, w, 1, 1)
        base = term if base is None else base + term
    base_ref[0] = base.astype(BF16)


def merge_kernel(
    base_ref, left_ref, right_ref, leaf_left_ref, leaf_right_ref, first_right_ref, out_left_ref,
    both_left_ref, both_right_ref,
):
    rank = base_ref.shape[-1]
    for i in range(2):
        both_left_ref[i] = dot(leaf_left_ref[i], base_ref[0]).astype(BF16)
        out_left_ref[i] = dot(leaf_left_ref[i], left_ref[0]).astype(BF16)
        both_right_ref[i, :, :rank] = dot(leaf_right_ref[i], right_ref[0]).astype(BF16)
        both_right_ref[i, :, rank : 2 * rank] = leaf_right_ref[i]
        both_right_ref[i, :, 2 * rank :] = first_right_ref[i]


def final_kernel(
    position_ref, last_ref, other_last_ref, part_ref, first_left_ref, left_ref, base_ref, right_ref,
    out_hbm, out, sems,
):
    odd = (position_ref[0] & 1) == 1
    f = pick(odd, last_ref, other_last_ref, 0)
    first = pick(odd, other_last_ref, last_ref, 0)
    rows = part_ref.shape[1] // CHUNKS
    copies = []
    lasts = [dot(left_ref[i], f).astype(BF16) for i in range(2)]
    firsts = [dot(first_left_ref[i], first).astype(BF16) for i in range(2)]
    for i in range(2):
        e = jnp.concatenate([lasts[i], base_ref[i], firsts[i]], 1)
        for c in range(CHUNKS):
            here = pl.ds(c * rows, rows)
            full = part_ref[i, here] + contract(e[c * rows : (c + 1) * rows], right_ref[i], 1, 1)
            out[i, here] = full.astype(BF16)
            k = i * CHUNKS + c
            copies.append(pltpu.make_async_copy(out.at[i, here], out_hbm.at[i, here], sems.at[k]))
            copies[-1].start()
    for copy in copies:
        copy.wait()


def in_vmem(n, scalar=True):
    specs = [pl.BlockSpec(memory_space=VMEM)] * n
    return [pl.BlockSpec(memory_space=pltpu.SMEM)] + specs if scalar else specs


def small(mib=2):
    return pltpu.CompilerParams(vmem_limit_bytes=mib << 20)


def exchange(block, count, odd_bit, even_bit):
    route = [(p, p ^ (1 << (odd_bit if p & 1 else even_bit))) for p in range(count)]
    return lax.ppermute(block, AXES, route)


def stages(dense_a, dense_b, inner_basis_stack, outer_basis_stack, ascent, descent, couplings):
    count = lax.axis_size("row") * lax.axis_size("col")
    levels = count.bit_length() - 1
    rank = ascent.shape[-1]
    place = lax.axis_index(AXES).reshape(1).astype(jnp.int32)

    def mats(n):
        return jax.ShapeDtypeStruct((n, rank, rank), BF16)

    tall = jax.ShapeDtypeStruct(outer_basis_stack.shape[:1] + outer_basis_stack.shape[2:], BF16)

    wide = jax.ShapeDtypeStruct(tall.shape[:2] + (3 * rank,), BF16)
    whole = jax.ShapeDtypeStruct(dense_a.shape, F32)

    def call(kernel, outs, *refs, scalar=True, mib=2):
        outs = tuple(mats(n) if isinstance(n, int) else n for n in outs)
        return pl.pallas_call(
            kernel,
            out_shape=outs,
            in_specs=in_vmem(len(refs), scalar),
            out_specs=tuple(in_vmem(len(outs), False)),
            compiler_params=small(mib),
        )(*([place] if scalar else []), *refs)

    send, pq, swk, leaf_inner = pl.pallas_call(
        functools.partial(head_kernel, levels),
        out_shape=(mats(4), mats(2), mats(6), mats(2)),
        in_specs=[pl.BlockSpec(memory_space=pltpu.SMEM)]
        + [pl.BlockSpec(memory_space=pltpu.HBM)] * 4,
        out_specs=tuple(in_vmem(4, False)),
        scratch_shapes=[
            VMEM(inner_basis_stack.shape, BF16),
            VMEM((3, 2, rank, rank), BF16),
            pltpu.SemaphoreType.DMA((6,)),
        ],
        compiler_params=small(4),
        name="head",
    )(place, *[
        pltpu.with_memory_space_constraint(x, pltpu.HBM)
        for x in (inner_basis_stack, ascent, descent, couplings)
    ])
    dense = pl.pallas_call(
        dense_kernel,
        out_shape=jax.ShapeDtypeStruct(dense_a.shape, F32),
        in_specs=in_vmem(2, False),
        out_specs=in_vmem(1, False)[0],
        compiler_params=small(8),
        name="dense",
    )(dense_a, dense_b)

    def width(r):
        climbing = 3 if r == 1 else 4 if r <= levels - 2 else 1
        return climbing if r in (1, levels - 1) else max(climbing, sent(r - 1, levels))

    got = exchange(send, count, 0, 0)
    block, first = call(functools.partial(start_kernel, levels), (width(1), 1), send, got, pq, swk)
    carry = other_swk = exchange(swk, count, 0, 0)
    part, left, right, first, first_left, first_right = call(
        prepare_kernel, (whole, tall, tall, 1, tall, tall), got, swk, other_swk, first,
        leaf_inner, descent, couplings, dense, outer_basis_stack, mib=12,
    )
    received, nodes = [], []
    for r in range(1, levels - 1):
        new = exchange(block, count, r, levels - 2 if r == 1 else r - 1)
        if r > 1:
            received.append(new)
        outs = (width(r + 1), 4 if r == levels - 2 else 6) + ((4,) if r > 1 else ())
        kernel = functools.partial(round_kernel, r, levels)
        more = (first,) if r == levels - 2 else ()
        block, carry, *node = call(kernel, outs, block, new, carry, *more)
        nodes += node
    last = exchange(block, count, levels - 1, 1)

    size = 4 * len(nodes) + 4
    kernel = functools.partial(pack_kernel, len(received))
    (mine,) = call(kernel, (size,), *received, *nodes, carry)
    other = exchange(mine, count, 0, 0)
    kernel = functools.partial(upper_kernel, levels)
    upper_terms = call(kernel, (1, 1, 1), swk, other_swk, mine, other)
    sides = call(
        merge_kernel, (tall, tall, wide), *upper_terms, left, right, first_right,
        scalar=False, mib=4,
    )
    other_last = exchange(last, count, 0, 0)

    return pl.pallas_call(
        final_kernel,
        out_shape=jax.ShapeDtypeStruct(dense.shape, BF16),
        in_specs=in_vmem(7),
        out_specs=pl.BlockSpec(memory_space=pltpu.HBM),
        scratch_shapes=[VMEM(dense.shape, BF16), pltpu.SemaphoreType.DMA((2 * CHUNKS,))],
        compiler_params=small(12),
        name="final",
    )(place, last, other_last, part, first_left, *sides)


def solution(mesh):
    placed = (
        P(AXES, None, None),
        P(AXES, None, None),
        P(AXES, None, None, None),
        P(AXES, None, None, None),
        P(AXES, None, None, None, None),
        P(AXES, None, None, None, None),
        P(AXES, None, None, None, None),
    )
    return jax.shard_map(
        stages, mesh=mesh, in_specs=placed, out_specs=P(AXES, None, None), check_vma=False
    )
```

```python
import functools

import jax
import jax.numpy as jnp
from jax import lax
from jax.experimental import pallas as pl
from jax.experimental.pallas import tpu as pltpu
from jax.sharding import PartitionSpec as P

AXES = ("row", "col")
BF16 = jnp.bfloat16
F32 = jnp.float32
VMEM = pltpu.VMEM
CHUNKS = 2


def contract(a, b, left, right):
    return lax.dot_general(a, b, (((left,), (right,)), ((), ())), preferred_element_type=F32)


def dot(a, b):
    return contract(a, b, 1, 0)


def lift(p, f, q):
    return dot(contract(p, f, 0, 0).astype(BF16), q)


def couple(k, f, k2):
    return dot(dot(k, f).astype(BF16), k2)


def lower(s, g, w):
    return contract(dot(s, g).astype(BF16), w, 1, 1)


def pick(first, first_ref, second_ref, i):
    return jnp.where(first, first_ref[i], second_ref[i])


def head_kernel(
    levels, position_ref, inner_hbm, up_hbm, down_hbm, block_hbm,
    send_ref, pq_ref, swk_ref, leaf_ref, inner, up, sems,
):
    copies = [
        pltpu.make_async_copy(up_hbm.at[0, 0:3], up, sems.at[0]),
        pltpu.make_async_copy(inner_hbm.at[0], inner.at[0], sems.at[1]),
        pltpu.make_async_copy(inner_hbm.at[1], inner.at[1], sems.at[2]),
        pltpu.make_async_copy(up_hbm.at[0, 3], pq_ref, sems.at[3]),
        pltpu.make_async_copy(down_hbm.at[0, 3], swk_ref.at[0:2], sems.at[4]),
        pltpu.make_async_copy(block_hbm.at[0, 1], swk_ref.at[2:6], sems.at[5]),
    ]
    for copy in copies:
        copy.start()
    copies[0].wait()
    twice = [[dot(up[i, k], up[2, k]).astype(BF16) for k in range(2)] for i in range(2)]
    leaves = []
    for i in range(2):
        copies[1 + i].wait()
        leaves.append(contract(inner[i, 0], inner[i, 1], 0, 0).astype(BF16))
        leaf_ref[i] = leaves[i]
    halves = [
        (contract(up[i, 0], leaves[i], 0, 0).astype(BF16),
         contract(twice[i][0], leaves[i], 0, 0).astype(BF16))
        for i in range(2)
    ]
    f = [dot(halves[i][0], up[i, 1]) for i in range(2)]
    t = [dot(halves[i][1], twice[i][1]) for i in range(2)]
    send_ref[0] = (f[0] + f[1]).astype(BF16)
    send_ref[1] = (t[0] + t[1]).astype(BF16)
    for copy in copies[3:]:
        copy.wait()
    odd = (position_ref[0] & 1) == 1
    high = (position_ref[0] >> (levels - 2)) & 1
    send_ref[2] = jnp.where(odd, swk_ref[3 - high], pq_ref[0])
    send_ref[3] = jnp.where(odd, swk_ref[4 + high], pq_ref[1])


def climb(low, r, levels, send_ref, got_ref, out_ref):
    t = 0 if r == 1 else 1
    f = (send_ref[t].astype(F32) + got_ref[t].astype(F32)).astype(BF16)
    out_ref[0] = f
    if r + 1 < levels - 1:
        p = pick(low, send_ref, got_ref, t + 1)
        q = pick(low, send_ref, got_ref, t + 2)
        out_ref[1] = lift(p, f, q).astype(BF16)
        out_ref[2] = pick(low, got_ref, send_ref, t + 1)
        out_ref[3] = pick(low, got_ref, send_ref, t + 2)


def start_kernel(levels, position_ref, send_ref, got_ref, pq_ref, swk_ref, out_ref, f_ref):
    position = position_ref[0]
    odd = (position & 1) == 1
    root = position == (1 << (levels - 1)) - 1
    f = (send_ref[1].astype(F32) + got_ref[1].astype(F32)).astype(BF16)
    f_ref[0] = f

    @pl.when(odd)
    def _():
        out_ref[0] = lift(got_ref[2], f, got_ref[3]).astype(BF16)
        out_ref[1] = jnp.where(root, swk_ref[3], pq_ref[0])
        out_ref[2] = jnp.where(root, swk_ref[4], pq_ref[1])

    @pl.when(jnp.logical_not(odd))
    def _():
        out_ref[0:2] = got_ref[2:4]


def sent(j, levels):
    return 6 if j <= levels - 4 else 4


def fill(j, levels, position, carry_ref, out_ref):
    if sent(j, levels) == 6:
        out_ref[0:6] = carry_ref[...]
        return
    low = ((position >> j) & 1) == 0

    @pl.when(low)
    def _():
        out_ref[0:2] = carry_ref[0:2]
        out_ref[2:4] = carry_ref[3:5]

    @pl.when(jnp.logical_not(low))
    def _():
        out_ref[0:4] = carry_ref[2:6]


def round_kernel(r, levels, position_ref, send_ref, got_ref, carry_ref, *refs):
    if r == levels - 2:
        first_ref, out_ref, new_ref, *node_refs = refs
    else:
        out_ref, new_ref, *node_refs = refs
    position = position_ref[0]
    odd = (position & 1) == 1

    @pl.when(odd)
    def _():
        low = ((position >> r) & 1) == 0
        climb(low, r, levels, send_ref, got_ref, out_ref)
        if r == levels - 2:
            @pl.when(((position >> (levels - 1)) & 1) == 0)
            def _():
                k1 = pick(low, got_ref, send_ref, 2)
                k2 = pick(low, got_ref, send_ref, 3)
                out_ref[0] = couple(k1, out_ref[0], k2).astype(BF16)

    @pl.when(jnp.logical_not(odd))
    def _():
        if r == 1:
            mask = (1 << (levels - 3)) - 1
            top = ((position >> 1) & mask) == mask
            new_ref[...] = carry_ref[...]

            @pl.when(top)
            def _():
                low = ((position >> (levels - 2)) & 1) == 0
                for i, own in ((0, 2), (1, 5)):
                    new_ref[2 + i] = jnp.where(low, carry_ref[own], got_ref[i])
                    new_ref[4 + i] = jnp.where(low, got_ref[i], carry_ref[own])

            fill(1, levels, position, new_ref, out_ref)
            return
        j = r - 1
        (node_ref,) = node_refs
        low = ((position >> j) & 1) == 0
        full = sent(j, levels) == 6

        @pl.when(low)
        def _():
            node_ref[0:3] = carry_ref[0:3]
            node_ref[3] = carry_ref[5]
            new_ref[...] = got_ref[0 : new_ref.shape[0]]

        @pl.when(jnp.logical_not(low))
        def _():
            node_ref[0:2] = got_ref[0:2]
            node_ref[2:4] = got_ref[3:5] if full else got_ref[2:4]
            new_ref[...] = carry_ref[...] if full else carry_ref[2:6]

        if full:
            fill(j + 1, levels, position, new_ref, out_ref)
        if r == levels - 2:
            out_ref[0] = first_ref[0]


def pack_kernel(count, position_ref, *refs):
    odd = (position_ref[0] & 1) == 1
    received, nodes, top_ref, out_ref = refs[:count], refs[count:-2], refs[-2], refs[-1]

    @pl.when(odd)
    def _():
        for i, ref in enumerate(received):
            out_ref[i] = ref[0]

    @pl.when(jnp.logical_not(odd))
    def _():
        for i, ref in enumerate(nodes):
            out_ref[4 * i : 4 * i + 4] = ref[...]
        out_ref[4 * len(nodes) : 4 * len(nodes) + 4] = top_ref[...]


def dense_kernel(a_ref, b_ref, o_ref):
    for i in range(2):
        o_ref[i] = dot(a_ref[i], b_ref[i])


def first_node(odd, swk_ref, other_swk_ref, i):
    left, right = ((0, 0), (1, 1), (2, 3), (5, 4))[i]
    return jnp.where(odd, other_swk_ref[right], swk_ref[left])


def prepare_kernel(
    position_ref, got_ref, swk_ref, other_swk_ref, f_ref, leaf_ref, down_ref, block_ref, dense_ref,
    outer_ref, out_ref, left_ref, right_ref, first_ref, first_left_ref, first_right_ref,
):
    odd = (position_ref[0] & 1) == 1
    low = ((position_ref[0] >> 1) & 1) == 0
    node = [pick(odd, swk_ref, other_swk_ref, k) for k in range(2, 6)]
    first_ref[0] = jnp.where(low, couple(node[1], f_ref[0], node[2]).astype(BF16), f_ref[0])
    near = couple(
        first_node(odd, swk_ref, other_swk_ref, 2),
        got_ref[0],
        first_node(odd, swk_ref, other_swk_ref, 3),
    ).astype(BF16)
    for i in range(2):
        s, w = down_ref[0, i, 0], down_ref[0, i, 1]
        leaf = couple(block_ref[0, 0, i], leaf_ref[1 - i], block_ref[0, 0, 3 - i])
        g = (leaf + lower(s, near, w)).astype(BF16)
        e = dot(outer_ref[i, 0], g).astype(BF16)
        out_ref[i] = dense_ref[i] + contract(e, outer_ref[i, 1], 1, 1)
        left = dot(s, down_ref[0, 2, 0]).astype(BF16)
        right = dot(w, down_ref[0, 2, 1]).astype(BF16)
        left = dot(outer_ref[i, 0], left).astype(BF16)
        right = dot(outer_ref[i, 1], right).astype(BF16)
        left_ref[i] = left
        right_ref[i] = right
        first_left_ref[i] = jnp.where(low, dot(left, node[0]).astype(BF16), left)
        first_right_ref[i] = jnp.where(low, contract(right, node[3], 1, 1).astype(BF16), right)


def upper_kernel(
    levels, position_ref, swk_ref, other_swk_ref, mine_ref, other_ref, base_ref, left_ref, right_ref
):
    position = position_ref[0]
    odd = (position & 1) == 1
    in_left = ((position >> (levels - 1)) & 1) == 0

    def inner(height):
        return pick(odd, mine_ref, other_ref, height - 2)

    def generator(height, i):
        if height == 1:
            return first_node(odd, swk_ref, other_swk_ref, i)
        slot = 4 * (height - 2) + i
        if height >= levels - 1:
            slot = 4 * (levels - 3) + 2 * (height - levels + 1) + i - 2
        return pick(odd, other_ref, mine_ref, slot)

    heights = range(3, levels)
    nears = [dot(generator(h, 2), inner(h - 1)).astype(BF16) for h in heights]
    sides = [(generator(1, 0), generator(1, 1))]
    for n, h in enumerate(heights):
        nears[n] = dot(nears[n], generator(h, 3)).astype(BF16)
        s, w = (dot(x, generator(h - 1, k)).astype(BF16) for k, x in enumerate(sides[-1]))
        sides.append((s, w))
    left, right = sides[-1]
    left_ref[0] = jnp.where(in_left, dot(left, generator(levels, 2)).astype(BF16), left)
    right_ref[0] = jnp.where(
        in_left, contract(right, generator(levels, 3), 1, 1).astype(BF16), right
    )
    halves = [dot(s, near).astype(BF16) for (s, _), near in zip(sides, nears)]
    base = None
    for half, (_, w) in zip(halves, sides):
        term = contract(half, w, 1, 1)
        base = term if base is None else base + term
    base_ref[0] = base.astype(BF16)


def merge_kernel(
    base_ref, left_ref, right_ref, part_ref, leaf_left_ref, leaf_right_ref, first_right_ref,
    out_ref, out_left_ref, both_right_ref,
):
    rank = base_ref.shape[-1]
    bases = [dot(leaf_left_ref[i], base_ref[0]).astype(BF16) for i in range(2)]
    for i in range(2):
        out_left_ref[i] = dot(leaf_left_ref[i], left_ref[0]).astype(BF16)
        both_right_ref[i, :, :rank] = dot(leaf_right_ref[i], right_ref[0]).astype(BF16)
        both_right_ref[i, :, rank:] = first_right_ref[i]
        out_ref[i] = part_ref[i] + contract(bases[i], leaf_right_ref[i], 1, 1)


def final_kernel(
    position_ref, last_ref, other_last_ref, first_left_ref, part_ref, left_ref, right_ref, out_hbm,
    out, sems,
):
    odd = (position_ref[0] & 1) == 1
    f = pick(odd, last_ref, other_last_ref, 0)
    first = pick(odd, other_last_ref, last_ref, 0)
    rows = part_ref.shape[1] // CHUNKS
    copies = []
    lasts = [dot(left_ref[i], f).astype(BF16) for i in range(2)]
    firsts = [dot(first_left_ref[i], first).astype(BF16) for i in range(2)]
    for i in range(2):
        e = jnp.concatenate([lasts[i], firsts[i]], 1)
        for c in range(CHUNKS):
            here = pl.ds(c * rows, rows)
            full = part_ref[i, here] + contract(e[c * rows : (c + 1) * rows], right_ref[i], 1, 1)
            out[i, here] = full.astype(BF16)
            k = i * CHUNKS + c
            copies.append(pltpu.make_async_copy(out.at[i, here], out_hbm.at[i, here], sems.at[k]))
            copies[-1].start()
    for copy in copies:
        copy.wait()


def in_vmem(n, scalar=True):
    specs = [pl.BlockSpec(memory_space=VMEM)] * n
    return [pl.BlockSpec(memory_space=pltpu.SMEM)] + specs if scalar else specs


def small(mib=2):
    return pltpu.CompilerParams(vmem_limit_bytes=mib << 20)


def exchange(block, count, odd_bit, even_bit):
    route = [(p, p ^ (1 << (odd_bit if p & 1 else even_bit))) for p in range(count)]
    return lax.ppermute(block, AXES, route)


def stages(dense_a, dense_b, inner_basis_stack, outer_basis_stack, ascent, descent, couplings):
    count = lax.axis_size("row") * lax.axis_size("col")
    levels = count.bit_length() - 1
    rank = ascent.shape[-1]
    place = lax.axis_index(AXES).reshape(1).astype(jnp.int32)

    def mats(n):
        return jax.ShapeDtypeStruct((n, rank, rank), BF16)

    tall = jax.ShapeDtypeStruct(outer_basis_stack.shape[:1] + outer_basis_stack.shape[2:], BF16)

    wide = jax.ShapeDtypeStruct(tall.shape[:2] + (2 * rank,), BF16)
    whole = jax.ShapeDtypeStruct(dense_a.shape, F32)

    def call(kernel, outs, *refs, scalar=True, mib=2):
        outs = tuple(mats(n) if isinstance(n, int) else n for n in outs)
        return pl.pallas_call(
            kernel,
            out_shape=outs,
            in_specs=in_vmem(len(refs), scalar),
            out_specs=tuple(in_vmem(len(outs), False)),
            compiler_params=small(mib),
        )(*([place] if scalar else []), *refs)

    send, pq, swk, leaf_inner = pl.pallas_call(
        functools.partial(head_kernel, levels),
        out_shape=(mats(4), mats(2), mats(6), mats(2)),
        in_specs=[pl.BlockSpec(memory_space=pltpu.SMEM)]
        + [pl.BlockSpec(memory_space=pltpu.HBM)] * 4,
        out_specs=tuple(in_vmem(4, False)),
        scratch_shapes=[
            VMEM(inner_basis_stack.shape, BF16),
            VMEM((3, 2, rank, rank), BF16),
            pltpu.SemaphoreType.DMA((6,)),
        ],
        compiler_params=small(4),
        name="head",
    )(place, *[
        pltpu.with_memory_space_constraint(x, pltpu.HBM)
        for x in (inner_basis_stack, ascent, descent, couplings)
    ])
    dense = pl.pallas_call(
        dense_kernel,
        out_shape=jax.ShapeDtypeStruct(dense_a.shape, F32),
        in_specs=in_vmem(2, False),
        out_specs=in_vmem(1, False)[0],
        compiler_params=small(8),
        name="dense",
    )(dense_a, dense_b)

    def width(r):
        climbing = 3 if r == 1 else 4 if r <= levels - 2 else 1
        return climbing if r in (1, levels - 1) else max(climbing, sent(r - 1, levels))

    got = exchange(send, count, 0, 0)
    block, first = call(functools.partial(start_kernel, levels), (width(1), 1), send, got, pq, swk)
    carry = other_swk = exchange(swk, count, 0, 0)
    part, left, right, first, first_left, first_right = call(
        prepare_kernel, (whole, tall, tall, 1, tall, tall), got, swk, other_swk, first,
        leaf_inner, descent, couplings, dense, outer_basis_stack, mib=12,
    )
    received, nodes = [], []
    for r in range(1, levels - 1):
        new = exchange(block, count, r, levels - 2 if r == 1 else r - 1)
        if r > 1:
            received.append(new)
        outs = (width(r + 1), 4 if r == levels - 2 else 6) + ((4,) if r > 1 else ())
        kernel = functools.partial(round_kernel, r, levels)
        more = (first,) if r == levels - 2 else ()
        block, carry, *node = call(kernel, outs, block, new, carry, *more)
        nodes += node
    last = exchange(block, count, levels - 1, 1)

    size = 4 * len(nodes) + 4
    kernel = functools.partial(pack_kernel, len(received))
    (mine,) = call(kernel, (size,), *received, *nodes, carry)
    other = exchange(mine, count, 0, 0)
    kernel = functools.partial(upper_kernel, levels)
    upper_terms = call(kernel, (1, 1, 1), swk, other_swk, mine, other)
    sides = call(
        merge_kernel, (whole, tall, wide), *upper_terms, part, left, right, first_right,
        scalar=False, mib=12,
    )
    other_last = exchange(last, count, 0, 0)

    return pl.pallas_call(
        final_kernel,
        out_shape=jax.ShapeDtypeStruct(dense.shape, BF16),
        in_specs=in_vmem(6),
        out_specs=pl.BlockSpec(memory_space=pltpu.HBM),
        scratch_shapes=[VMEM(dense.shape, BF16), pltpu.SemaphoreType.DMA((2 * CHUNKS,))],
        compiler_params=small(12),
        name="final",
    )(place, last, other_last, first_left, *sides)


def solution(mesh):
    placed = (
        P(AXES, None, None),
        P(AXES, None, None),
        P(AXES, None, None, None),
        P(AXES, None, None, None),
        P(AXES, None, None, None, None),
        P(AXES, None, None, None, None),
        P(AXES, None, None, None, None),
    )
    return jax.shard_map(
        stages, mesh=mesh, in_specs=placed, out_specs=P(AXES, None, None), check_vma=False
    )
```

```python
import functools

import jax
import jax.numpy as jnp
from jax import lax
from jax.experimental import pallas as pl
from jax.experimental.pallas import tpu as pltpu
from jax.sharding import PartitionSpec as P

AXES = ("row", "col")
BF16 = jnp.bfloat16
F32 = jnp.float32
VMEM = pltpu.VMEM
CHUNKS = 2


def contract(a, b, left, right):
    return lax.dot_general(a, b, (((left,), (right,)), ((), ())), preferred_element_type=F32)


def dot(a, b):
    return contract(a, b, 1, 0)


def lift(p, f, q):
    return dot(contract(p, f, 0, 0).astype(BF16), q)


def couple(k, f, k2):
    return dot(dot(k, f).astype(BF16), k2)


def lower(s, g, w):
    return contract(dot(s, g).astype(BF16), w, 1, 1)


def pick(first, first_ref, second_ref, i):
    return jnp.where(first, first_ref[i], second_ref[i])


def head_kernel(
    levels, position_ref, inner_hbm, up_hbm, down_hbm, block_hbm,
    send_ref, pq_ref, swk_ref, leaf_ref, inner, up, sems,
):
    copies = [
        pltpu.make_async_copy(up_hbm.at[0, 0:3], up, sems.at[0]),
        pltpu.make_async_copy(inner_hbm.at[0], inner.at[0], sems.at[1]),
        pltpu.make_async_copy(inner_hbm.at[1], inner.at[1], sems.at[2]),
        pltpu.make_async_copy(up_hbm.at[0, 3], pq_ref, sems.at[3]),
        pltpu.make_async_copy(down_hbm.at[0, 3], swk_ref.at[0:2], sems.at[4]),
        pltpu.make_async_copy(block_hbm.at[0, 1], swk_ref.at[2:6], sems.at[5]),
    ]
    for copy in copies:
        copy.start()
    copies[0].wait()
    twice = [[dot(up[i, k], up[2, k]).astype(BF16) for k in range(2)] for i in range(2)]
    leaves = []
    for i in range(2):
        copies[1 + i].wait()
        leaves.append(contract(inner[i, 0], inner[i, 1], 0, 0).astype(BF16))
        leaf_ref[i] = leaves[i]
    halves = [
        (contract(up[i, 0], leaves[i], 0, 0).astype(BF16),
         contract(twice[i][0], leaves[i], 0, 0).astype(BF16))
        for i in range(2)
    ]
    f = [dot(halves[i][0], up[i, 1]) for i in range(2)]
    t = [dot(halves[i][1], twice[i][1]) for i in range(2)]
    send_ref[0] = (f[0] + f[1]).astype(BF16)
    send_ref[1] = (t[0] + t[1]).astype(BF16)
    for copy in copies[3:]:
        copy.wait()
    odd = (position_ref[0] & 1) == 1
    high = (position_ref[0] >> (levels - 2)) & 1
    send_ref[2] = jnp.where(odd, swk_ref[3 - high], pq_ref[0])
    send_ref[3] = jnp.where(odd, swk_ref[4 + high], pq_ref[1])


def climb(low, r, levels, send_ref, got_ref, out_ref):
    t = 0 if r == 1 else 1
    f = (send_ref[t].astype(F32) + got_ref[t].astype(F32)).astype(BF16)
    out_ref[0] = f
    if r + 1 < levels - 1:
        p = pick(low, send_ref, got_ref, t + 1)
        q = pick(low, send_ref, got_ref, t + 2)
        out_ref[1] = lift(p, f, q).astype(BF16)
        out_ref[2] = pick(low, got_ref, send_ref, t + 1)
        out_ref[3] = pick(low, got_ref, send_ref, t + 2)


def start_kernel(levels, position_ref, send_ref, got_ref, pq_ref, swk_ref, out_ref, f_ref):
    position = position_ref[0]
    odd = (position & 1) == 1
    root = position == (1 << (levels - 1)) - 1
    f = (send_ref[1].astype(F32) + got_ref[1].astype(F32)).astype(BF16)
    f_ref[0] = f

    @pl.when(odd)
    def _():
        out_ref[0] = lift(got_ref[2], f, got_ref[3]).astype(BF16)
        out_ref[1] = jnp.where(root, swk_ref[3], pq_ref[0])
        out_ref[2] = jnp.where(root, swk_ref[4], pq_ref[1])

    @pl.when(jnp.logical_not(odd))
    def _():
        out_ref[0:2] = got_ref[2:4]


def sent(j, levels):
    return 6 if j <= levels - 4 else 4


def fill(j, levels, position, carry_ref, out_ref):
    if sent(j, levels) == 6:
        out_ref[0:6] = carry_ref[...]
        return
    low = ((position >> j) & 1) == 0

    @pl.when(low)
    def _():
        out_ref[0:2] = carry_ref[0:2]
        out_ref[2:4] = carry_ref[3:5]

    @pl.when(jnp.logical_not(low))
    def _():
        out_ref[0:4] = carry_ref[2:6]


def round_kernel(r, levels, position_ref, send_ref, got_ref, carry_ref, *refs):
    if r == levels - 2:
        first_ref, out_ref, new_ref, *node_refs = refs
    else:
        out_ref, new_ref, *node_refs = refs
    position = position_ref[0]
    odd = (position & 1) == 1

    @pl.when(odd)
    def _():
        low = ((position >> r) & 1) == 0
        climb(low, r, levels, send_ref, got_ref, out_ref)
        if r == levels - 2:
            @pl.when(((position >> (levels - 1)) & 1) == 0)
            def _():
                k1 = pick(low, got_ref, send_ref, 2)
                k2 = pick(low, got_ref, send_ref, 3)
                out_ref[0] = couple(k1, out_ref[0], k2).astype(BF16)

    @pl.when(jnp.logical_not(odd))
    def _():
        if r == 1:
            mask = (1 << (levels - 3)) - 1
            top = ((position >> 1) & mask) == mask
            new_ref[...] = carry_ref[...]

            @pl.when(top)
            def _():
                low = ((position >> (levels - 2)) & 1) == 0
                for i, own in ((0, 2), (1, 5)):
                    new_ref[2 + i] = jnp.where(low, carry_ref[own], got_ref[i])
                    new_ref[4 + i] = jnp.where(low, got_ref[i], carry_ref[own])

            fill(1, levels, position, new_ref, out_ref)
            return
        j = r - 1
        (node_ref,) = node_refs
        low = ((position >> j) & 1) == 0
        full = sent(j, levels) == 6

        @pl.when(low)
        def _():
            node_ref[0:3] = carry_ref[0:3]
            node_ref[3] = carry_ref[5]
            new_ref[...] = got_ref[0 : new_ref.shape[0]]

        @pl.when(jnp.logical_not(low))
        def _():
            node_ref[0:2] = got_ref[0:2]
            node_ref[2:4] = got_ref[3:5] if full else got_ref[2:4]
            new_ref[...] = carry_ref[...] if full else carry_ref[2:6]

        if full:
            fill(j + 1, levels, position, new_ref, out_ref)
        if r == levels - 2:
            out_ref[0] = first_ref[0]


def pack_kernel(count, position_ref, *refs):
    odd = (position_ref[0] & 1) == 1
    received, nodes, top_ref, out_ref = refs[:count], refs[count:-2], refs[-2], refs[-1]

    @pl.when(odd)
    def _():
        for i, ref in enumerate(received):
            out_ref[i] = ref[0]

    @pl.when(jnp.logical_not(odd))
    def _():
        for i, ref in enumerate(nodes):
            out_ref[4 * i : 4 * i + 4] = ref[...]
        out_ref[4 * len(nodes) : 4 * len(nodes) + 4] = top_ref[...]


def dense_kernel(a_ref, b_ref, o_ref):
    for i in range(2):
        o_ref[i] = dot(a_ref[i], b_ref[i])


def first_node(odd, swk_ref, other_swk_ref, i):
    left, right = ((0, 0), (1, 1), (2, 3), (5, 4))[i]
    return jnp.where(odd, other_swk_ref[right], swk_ref[left])


def prepare_kernel(
    position_ref, got_ref, swk_ref, other_swk_ref, f_ref, leaf_ref, down_ref, block_ref, dense_ref,
    outer_ref, out_ref, left_ref, right_ref, first_ref, first_left_ref, first_right_ref,
):
    odd = (position_ref[0] & 1) == 1
    low = ((position_ref[0] >> 1) & 1) == 0
    node = [pick(odd, swk_ref, other_swk_ref, k) for k in range(2, 6)]
    first_ref[0] = jnp.where(low, couple(node[1], f_ref[0], node[2]).astype(BF16), f_ref[0])
    near = couple(
        first_node(odd, swk_ref, other_swk_ref, 2),
        got_ref[0],
        first_node(odd, swk_ref, other_swk_ref, 3),
    ).astype(BF16)
    for i in range(2):
        s, w = down_ref[0, i, 0], down_ref[0, i, 1]
        leaf = couple(block_ref[0, 0, i], leaf_ref[1 - i], block_ref[0, 0, 3 - i])
        g = (leaf + lower(s, near, w)).astype(BF16)
        e = dot(outer_ref[i, 0], g).astype(BF16)
        out_ref[i] = dense_ref[i] + contract(e, outer_ref[i, 1], 1, 1)
        left = dot(s, down_ref[0, 2, 0]).astype(BF16)
        right = dot(w, down_ref[0, 2, 1]).astype(BF16)
        left = dot(outer_ref[i, 0], left).astype(BF16)
        right = dot(outer_ref[i, 1], right).astype(BF16)
        left_ref[i] = left
        right_ref[i] = right
        first_left_ref[i] = jnp.where(low, dot(left, node[0]).astype(BF16), left)
        first_right_ref[i] = jnp.where(low, contract(right, node[3], 1, 1).astype(BF16), right)


def upper_kernel(
    levels, position_ref, swk_ref, other_swk_ref, mine_ref, other_ref, base_ref, left_ref, right_ref
):
    position = position_ref[0]
    odd = (position & 1) == 1
    in_left = ((position >> (levels - 1)) & 1) == 0

    def inner(height):
        return pick(odd, mine_ref, other_ref, height - 2)

    def generator(height, i):
        if height == 1:
            return first_node(odd, swk_ref, other_swk_ref, i)
        slot = 4 * (height - 2) + i
        if height >= levels - 1:
            slot = 4 * (levels - 3) + 2 * (height - levels + 1) + i - 2
        return pick(odd, other_ref, mine_ref, slot)

    heights = range(3, levels)
    nears = [dot(generator(h, 2), inner(h - 1)).astype(BF16) for h in heights]
    sides = [(generator(1, 0), generator(1, 1))]
    for n, h in enumerate(heights):
        nears[n] = dot(nears[n], generator(h, 3)).astype(BF16)
        s, w = (dot(x, generator(h - 1, k)).astype(BF16) for k, x in enumerate(sides[-1]))
        sides.append((s, w))
    left, right = sides[-1]
    left_ref[0] = jnp.where(in_left, dot(left, generator(levels, 2)).astype(BF16), left)
    right_ref[0] = jnp.where(
        in_left, contract(right, generator(levels, 3), 1, 1).astype(BF16), right
    )
    halves = [dot(s, near).astype(BF16) for (s, _), near in zip(sides, nears)]
    base = None
    for half, (_, w) in zip(halves, sides):
        term = contract(half, w, 1, 1)
        base = term if base is None else base + term
    base_ref[0] = base.astype(BF16)


def merge_kernel(
    base_ref, left_ref, right_ref, part_ref, leaf_left_ref, leaf_right_ref, first_right_ref,
    out_ref, out_left_ref, both_right_ref,
):
    rank = base_ref.shape[-1]
    for i in range(2):
        out_left_ref[i] = dot(leaf_left_ref[i], left_ref[0]).astype(BF16)
        both_right_ref[i, :, :rank] = dot(leaf_right_ref[i], right_ref[0]).astype(BF16)
        both_right_ref[i, :, rank:] = first_right_ref[i]
    bases = [dot(leaf_left_ref[i], base_ref[0]).astype(BF16) for i in range(2)]
    for i in range(2):
        out_ref[i] = part_ref[i] + contract(bases[i], leaf_right_ref[i], 1, 1)


def top_kernel(levels, *refs):
    upper_kernel(levels, *refs[:5], *refs[-3:])
    merge_kernel(*refs[-3:], *refs[5:-3])


def final_kernel(
    position_ref, last_ref, other_last_ref, first_left_ref, part_ref, left_ref, right_ref, out_hbm,
    out, sems,
):
    odd = (position_ref[0] & 1) == 1
    f = pick(odd, last_ref, other_last_ref, 0)
    first = pick(odd, other_last_ref, last_ref, 0)
    rows = part_ref.shape[1] // CHUNKS
    copies = []
    lasts = [dot(left_ref[i], f).astype(BF16) for i in range(2)]
    firsts = [dot(first_left_ref[i], first).astype(BF16) for i in range(2)]
    for i in range(2):
        e = jnp.concatenate([lasts[i], firsts[i]], 1)
        for c in range(CHUNKS):
            here = pl.ds(c * rows, rows)
            full = part_ref[i, here] + contract(e[c * rows : (c + 1) * rows], right_ref[i], 1, 1)
            out[i, here] = full.astype(BF16)
            k = i * CHUNKS + c
            copies.append(pltpu.make_async_copy(out.at[i, here], out_hbm.at[i, here], sems.at[k]))
            copies[-1].start()
    for copy in copies:
        copy.wait()


def in_vmem(n, scalar=True):
    specs = [pl.BlockSpec(memory_space=VMEM)] * n
    return [pl.BlockSpec(memory_space=pltpu.SMEM)] + specs if scalar else specs


def small(mib=2):
    return pltpu.CompilerParams(vmem_limit_bytes=mib << 20)


def exchange(block, count, odd_bit, even_bit):
    route = [(p, p ^ (1 << (odd_bit if p & 1 else even_bit))) for p in range(count)]
    return lax.ppermute(block, AXES, route)


def stages(dense_a, dense_b, inner_basis_stack, outer_basis_stack, ascent, descent, couplings):
    count = lax.axis_size("row") * lax.axis_size("col")
    levels = count.bit_length() - 1
    rank = ascent.shape[-1]
    place = lax.axis_index(AXES).reshape(1).astype(jnp.int32)

    def mats(n):
        return jax.ShapeDtypeStruct((n, rank, rank), BF16)

    tall = jax.ShapeDtypeStruct(outer_basis_stack.shape[:1] + outer_basis_stack.shape[2:], BF16)

    wide = jax.ShapeDtypeStruct(tall.shape[:2] + (2 * rank,), BF16)
    whole = jax.ShapeDtypeStruct(dense_a.shape, F32)

    def call(kernel, outs, *refs, mib=2, scratch=0):
        outs = tuple(mats(n) if isinstance(n, int) else n for n in outs)
        return pl.pallas_call(
            kernel,
            out_shape=outs,
            in_specs=in_vmem(len(refs)),
            scratch_shapes=[VMEM((1, rank, rank), BF16)] * scratch,
            out_specs=tuple(in_vmem(len(outs), False)),
            compiler_params=small(mib),
        )(place, *refs)

    send, pq, swk, leaf_inner = pl.pallas_call(
        functools.partial(head_kernel, levels),
        out_shape=(mats(4), mats(2), mats(6), mats(2)),
        in_specs=[pl.BlockSpec(memory_space=pltpu.SMEM)]
        + [pl.BlockSpec(memory_space=pltpu.HBM)] * 4,
        out_specs=tuple(in_vmem(4, False)),
        scratch_shapes=[
            VMEM(inner_basis_stack.shape, BF16),
            VMEM((3, 2, rank, rank), BF16),
            pltpu.SemaphoreType.DMA((6,)),
        ],
        compiler_params=small(4),
        name="head",
    )(place, *[
        pltpu.with_memory_space_constraint(x, pltpu.HBM)
        for x in (inner_basis_stack, ascent, descent, couplings)
    ])
    dense = pl.pallas_call(
        dense_kernel,
        out_shape=jax.ShapeDtypeStruct(dense_a.shape, F32),
        in_specs=in_vmem(2, False),
        out_specs=in_vmem(1, False)[0],
        compiler_params=small(8),
        name="dense",
    )(dense_a, dense_b)

    def width(r):
        climbing = 3 if r == 1 else 4 if r <= levels - 2 else 1
        return climbing if r in (1, levels - 1) else max(climbing, sent(r - 1, levels))

    got = exchange(send, count, 0, 0)
    block, first = call(functools.partial(start_kernel, levels), (width(1), 1), send, got, pq, swk)
    carry = other_swk = exchange(swk, count, 0, 0)
    part, left, right, first, first_left, first_right = call(
        prepare_kernel, (whole, tall, tall, 1, tall, tall), got, swk, other_swk, first,
        leaf_inner, descent, couplings, dense, outer_basis_stack, mib=12,
    )
    received, nodes = [], []
    for r in range(1, levels - 1):
        new = exchange(block, count, r, levels - 2 if r == 1 else r - 1)
        if r > 1:
            received.append(new)
        outs = (width(r + 1), 4 if r == levels - 2 else 6) + ((4,) if r > 1 else ())
        kernel = functools.partial(round_kernel, r, levels)
        more = (first,) if r == levels - 2 else ()
        block, carry, *node = call(kernel, outs, block, new, carry, *more)
        nodes += node
    last = exchange(block, count, levels - 1, 1)

    size = 4 * len(nodes) + 4
    kernel = functools.partial(pack_kernel, len(received))
    (mine,) = call(kernel, (size,), *received, *nodes, carry)
    other = exchange(mine, count, 0, 0)
    kernel = functools.partial(top_kernel, levels)
    sides = call(
        kernel, (whole, tall, wide), swk, other_swk, mine, other, part, left, right,
        first_right, mib=12, scratch=3,
    )
    other_last = exchange(last, count, 0, 0)

    return pl.pallas_call(
        final_kernel,
        out_shape=jax.ShapeDtypeStruct(dense.shape, BF16),
        in_specs=in_vmem(6),
        out_specs=pl.BlockSpec(memory_space=pltpu.HBM),
        scratch_shapes=[VMEM(dense.shape, BF16), pltpu.SemaphoreType.DMA((2 * CHUNKS,))],
        compiler_params=small(12),
        name="final",
    )(place, last, other_last, first_left, *sides)


def solution(mesh):
    placed = (
        P(AXES, None, None),
        P(AXES, None, None),
        P(AXES, None, None, None),
        P(AXES, None, None, None),
        P(AXES, None, None, None, None),
        P(AXES, None, None, None, None),
        P(AXES, None, None, None, None),
    )
    return jax.shard_map(
        stages, mesh=mesh, in_specs=placed, out_specs=P(AXES, None, None), check_vma=False
    )
```
